32 devices in a mesh: row: 2 (over x), col: 16 (over z, y, core).
Axes of the slice: x: 2, y: 2, z: 4, core: 2. Of those that a mesh axis runs over, the one named last changes fastest.
Arguments:
- matrix: bfloat16 [1024, 65536], P('row', 'col'), may hold values from -0.1875 to 0.1875
- measured: float32 [256, 1024], P(None, 'row'), may hold values from -160 to 160
- support: int32 [4, 1024], replicated, may hold values from 0 to 65535, as said below
Outputs:
- estimate: float32 [256, 65536], P('row', 'col')
- row_norms: float32 [65536], P('col')
- residual_energy: float32 [4], replicated
The draws below stay inside these ranges and needn't reach their ends.
Inputs may be any that keep to these rules, and one draw needn't show every extreme that they name: Each row of support lists 1024 distinct signal-row indices in increasing order; in every row, each aligned block of 4096 indices (the signal rows of one index of col) holds at most 128 of them, and some block exactly 128.
All inputs are finite; a program needn't handle non-finite values.
Results may differ from the reference program's by a relative error of at most 0.015.
Values may be sent and summed in bfloat16 or wider, within the bound.
A program may use at most 64 MiB of HBM per device.

```python
import math
import jax
import jax.numpy as jnp
from jax import lax

MB = 512
NB = 4096
L = 256
KB = 64
ITERS = 4
M = 1024
N = 65536
K = 1024
N_ROW = 2
N_COL = 16


def draw_measured(key, part):
    key_base, key_rows, key_signals = jax.random.split(key, 3)
    position = jnp.arange(M, dtype=jnp.float32) / max(M - 1, 1)
    rising = math.log(3.0)
    values = jax.random.normal(key_base, (L, M), jnp.float32)
    values = jnp.clip(values, -5.0, 5.0)
    row_scale = jnp.exp(rising * position + jax.random.uniform(key_rows, (M,), jnp.float32) * math.log(10.0 / 3.0)) / 3.0
    signal_scale = jnp.exp(jax.random.uniform(key_signals, (L,), jnp.float32) * math.log(10.0)) / math.sqrt(10.0)
    return values * row_scale[None, :] * signal_scale[:, None]


def draw_support(key, part):
    blocks = N // NB

    def one_iteration(iteration_key):
        key_order, key_shift, key_ranks = jax.random.split(iteration_key, 3)
        block_order = jax.random.permutation(key_order, blocks)
        shifts = jax.random.randint(key_shift, (blocks // 2,), 0, KB + 1).at[0].set(KB)
        counts = jnp.zeros((blocks,), jnp.int32).at[block_order[0::2]].set(KB + shifts).at[block_order[1::2]].set(KB - shifts)
        rank_table = jax.vmap(lambda block_key: jax.random.permutation(block_key, NB))(jax.random.split(key_ranks, blocks))
        chosen = (rank_table < counts[:, None]).reshape(-1)
        return jnp.nonzero(chosen, size=K)[0].astype(jnp.int32)
    return jax.vmap(one_iteration)(jax.random.split(key, ITERS))


def shard_levels(key, extent, cuts, least, largest):
    factor_of = 1.0
    for dim, shards_of in cuts:
        steps = jax.random.uniform(jax.random.fold_in(jax.random.fold_in(key, 6), dim), (shards_of,), jnp.float32, least / len(cuts), largest / len(cuts))
        factor_of = factor_of * jnp.repeat(jnp.exp(steps), extent[dim] // shards_of).reshape((-1,) + (1,) * (len(extent) - 1 - dim))
    return factor_of


def scatter_about(own_key, extent, deviation, bound, cuts=(), kind=jnp.bfloat16):
    result = deviation * jax.random.normal(own_key, extent, jnp.float32)
    if cuts:
        result = result * shard_levels(own_key, extent, cuts, -0.22, 0.18)
    return jnp.clip(result, -bound, bound).astype(kind)


def setup_inputs(seed: int = 0) -> dict:
    key_of = jax.random.split(jax.random.key(seed), 4)
    return {
        "matrix": scatter_about(key_of[0], (M, N), M ** -0.5, 0.1875, ((0, 2), (1, 16))),
        "measured": draw_measured(jax.random.fold_in(key_of[3], 71), 0),
        "support": draw_support(jax.random.fold_in(key_of[3], 71), 0),
    }


STEP_SIZE = 0.25

def predict(matrix, current_half):

    def add_block(block, summed):
        start_col = (block * NB).astype(jnp.int32)
        columns = lax.dynamic_slice_in_dim(matrix, start_col, NB, 1)
        signal_cols = lax.dynamic_slice_in_dim(current_half, start_col, NB, 1)
        return summed + lax.dot_general(signal_cols, columns, (((1,), (1,)), ((), ())), preferred_element_type=jnp.float32)
    return lax.fori_loop(0, N_COL, add_block, jnp.zeros((L, MB * N_ROW), jnp.float32))

def descend(matrix, residual_half):

    def one_block(block):
        start_col = (block * NB).astype(jnp.int32)
        columns = lax.dynamic_slice_in_dim(matrix, start_col, NB, 1)
        summed = jnp.zeros((L, NB), jnp.float32)
        for group_index in range(N_ROW):
            part_sum = jnp.dot(residual_half[:, group_index * MB:(group_index + 1) * MB], columns[group_index * MB:(group_index + 1) * MB], preferred_element_type=jnp.float32)
            rounded = lax.optimization_barrier(part_sum.astype(jnp.bfloat16))
            summed = summed + rounded.astype(jnp.float32)
        return summed
    blocks_out = lax.map(one_block, jnp.arange(N_COL, dtype=jnp.int32))
    return jnp.transpose(blocks_out, (1, 0, 2)).reshape(L, N_COL * NB)

def reference(matrix, measured, support):
    total_cols = NB * N_COL
    current = jnp.zeros((L, total_cols), jnp.float32)
    energies = []
    stepped = current
    for iteration in range(ITERS):
        if iteration == 0:
            residual = measured
        else:
            residual = measured - predict(matrix, current.astype(jnp.bfloat16))
        energies.append(jnp.sum(residual * residual) / (L * MB * N_ROW))
        gradient = descend(matrix, residual.astype(jnp.bfloat16))
        stepped = current + STEP_SIZE * gradient
        keep_mask = jnp.zeros((total_cols,), jnp.float32).at[support[iteration]].set(1.0)
        current = stepped * keep_mask[None, :]
    row_norms = jnp.sqrt(lax.optimization_barrier(jnp.sum(stepped * stepped, axis=0)))
    return (current, row_norms, jnp.stack(energies))
```

```python
import functools

import jax
import jax.numpy as jnp
from jax import lax
from jax.experimental import pallas as pl
from jax.experimental.pallas import tpu as pltpu
from jax.sharding import PartitionSpec as P

MESH = pl.DeviceIdType.MESH
KMAX = 128
STEP_SIZE = 0.25
CHUNK = 512
BF = jnp.bfloat16
F32 = jnp.float32
NT = (((1,), (1,)), ((), ()))


def nn(a, b):
    return jnp.dot(a, b, preferred_element_type=F32)


def nt(a, b):
    return lax.dot_general(a, b, NT, preferred_element_type=F32)


def split(v):
    hi = v.astype(BF)
    return hi, (v - hi.astype(F32)).astype(BF)


def sizes(n_row, n_col, signals, mb, columns, iterations):
    chips = n_col // 2
    mine = signals // n_row // 2
    groups = max(1, min(mine // 16, chips))
    parts = chips // groups
    total = mb * n_row
    return dict(
        n_row=n_row, chips=chips, mine=mine, gs=groups, gm=parts, ps=mine // groups, pm=total // parts,
        mb=mb, columns=columns, iters=iterations, half=signals // n_row, signals=signals,
        gr=parts // n_row, ahead=(columns * 7 // 16) // CHUNK * CHUNK if n_row == 2 else 0,
    )


def kernel(
    s, supp_ref, meas_ref, a_ref, out_ref, sums_ref, en_ref,
    a_vm, meas_vm, mpiece, onehot, kept, part_send, part_recv, img, rs, res, fin, foth,
    cur_send, cur_recv, qsend, qrecv, a_peer, nrm_send, nrm_recv, e_send, e_recv, e_both,
    a_sem, m_sem, mp_sem, send, kept_recv, kept_core, part_sem, rs_sem, ag_sem, fin_sem, foth_sem,
    core_sem, q_sem, ap_sem, nrm_sem, e_sem,
):
    n_row, chips, mine, gs, gm, ps, pm = (s[k] for k in ("n_row", "chips", "mine", "gs", "gm", "ps", "pm"))
    mb, columns, iters, half, gr, ahead = (s[k] for k in ("mb", "columns", "iters", "half", "gr", "ahead"))
    x = lax.axis_index("row")
    col = lax.axis_index("col")
    chip = col // 2
    core = col % 2
    other = 1 - core
    counter = [0]
    sends = []

    def put(src, dst, recv, row, column):
        copy = pltpu.make_async_remote_copy(
            src_ref=src, dst_ref=dst, send_sem=send.at[counter[0]], recv_sem=recv,
            device_id={"row": row, "col": column}, device_id_type=MESH,
        )
        copy.start()
        counter[0] += 1
        sends.append(copy)

    def drain():
        for copy in sends:
            copy.wait_send()
        sends.clear()

    def took(ref, sem):
        pltpu.make_async_copy(ref, ref, sem).wait()

    def row_at(d):
        return lax.rem(x + d, n_row)

    def row_from(d):
        return lax.rem(x + n_row - d, n_row)

    def chip_at(k):
        return lax.rem(chip + k, chips)

    partner = chip * 2 + other

    strips = 4
    strip = mb // strips
    loads = [
        pltpu.make_async_copy(a_ref.at[pl.ds(i * strip, strip)], a_vm.at[pl.ds(i * strip, strip)], a_sem.at[i])
        for i in range(strips)
    ]
    for load in loads:
        load.start()
    meas_load = pltpu.make_async_copy(meas_ref, meas_vm, m_sem)
    meas_load.start()

    barrier = pltpu.get_barrier_semaphore()
    greeted = 0
    for d in range(n_row):
        for k in range(chips):
            if d or k:
                pl.semaphore_signal(
                    barrier, inc=1, device_id={"row": row_at(d), "col": chip_at(k) * 2 + core}, device_id_type=MESH
                )
                greeted += 1
        pl.semaphore_signal(barrier, inc=1, device_id={"row": row_at(d), "col": partner}, device_id_type=MESH)
        greeted += 1

    k_all = supp_ref.shape[1]
    lane_k = lax.broadcasted_iota(jnp.int32, (1, k_all), 1).astype(F32)
    slot_k = lax.broadcasted_iota(jnp.int32, (KMAX, k_all), 0).astype(F32)
    eye = lax.broadcasted_iota(jnp.int32, (KMAX, KMAX), 0) == lax.broadcasted_iota(jnp.int32, (KMAX, KMAX), 1)
    lane_n = lax.broadcasted_iota(jnp.int32, (1, columns), 1).astype(F32)

    def window(t, block):
        row = supp_ref[pl.ds(t, 1), :].astype(F32)
        start = (block * columns).astype(F32)
        below = jnp.sum((row < start).astype(F32), axis=1, keepdims=True)
        inside = (row >= start) & (row < start + columns)
        chosen = ((lane_k - below) == slot_k) & inside
        return jnp.sum(jnp.where(chosen, row + 1.0, 0.0), axis=1, keepdims=True) - 1.0

    def as_row(index):
        return jnp.sum(jnp.where(eye, index, 0.0), axis=0, keepdims=True)

    def marks(t):
        return (window(t, col) - (col * columns).astype(F32)) == lane_n

    def place_onehot(t):
        onehot[t] = jnp.where(marks(t), 1.0, 0.0).astype(BF)

    my_slots = pl.ds(pl.multiple_of(core * KMAX, KMAX), KMAX)

    def gather_kept(t):
        for i in range(strips):
            if t == 0:
                loads[i].wait()
            picked = nt(onehot[t], a_vm[i * strip:(i + 1) * strip, :])
            kept[t, x, my_slots, i * strip:(i + 1) * strip] = picked.astype(BF)

    def send_kept(t):
        mine_kept = kept.at[t, x, my_slots]
        put(mine_kept, mine_kept, kept_core.at[t, 0], x, partner)
        for d in range(1, n_row):
            put(mine_kept, mine_kept, kept_recv.at[t, d - 1], row_at(d), col)

    def relay_kept(t):
        for d in range(1, n_row):
            got = kept.at[t, row_from(d), my_slots]
            took(got, kept_recv.at[t, d - 1])
            put(got, got, kept_core.at[t, d], x, partner)

    def wait_kept(t):
        for d in range(n_row):
            took(kept.at[t, 0, pl.ds(0, KMAX)], kept_core.at[t, d])

    place_onehot(0)
    gather_kept(0)
    pl.semaphore_wait(barrier, greeted)
    send_kept(0)

    meas_load.wait()
    kept_mine = kept[0, x, my_slots, :]
    part = nt(meas_vm[...].astype(BF), kept_mine).astype(BF)
    for r in range(n_row):
        for c in range(2):
            base = r * half + c * mine
            part_send[r, c] = part[base:base + mine]
    for d in range(n_row):
        if d:
            put(part_send.at[row_at(d), core], part_recv.at[2 * d + core], part_sem, row_at(d), col)
        put(part_send.at[row_at(d), other], part_recv.at[2 * d + core], part_sem, row_at(d), partner)
    part_recv[core] = part_send[x, core]

    gi = chip // gm
    gj = lax.rem(chip, gm)
    owner_row = gj // gr
    piece_lane = pl.ds(pl.multiple_of(lax.rem(gj, gr) * pm, 128), pm)

    def piece_rows(r):
        return pl.ds(pl.multiple_of(r * half + core * mine + gi * ps, 8), ps)

    mp_from = counter[0]
    counter[0] += n_row - 1

    def mp_copy(d):
        return pltpu.make_async_remote_copy(
            src_ref=meas_ref.at[piece_rows(row_at(d)), piece_lane], dst_ref=mpiece,
            send_sem=send.at[mp_from + d - 1], recv_sem=mp_sem,
            device_id={"row": row_at(d), "col": col}, device_id_type=MESH,
        )

    @pl.when(owner_row == x)
    def _():
        pltpu.make_async_copy(meas_ref.at[piece_rows(x), piece_lane], mpiece, mp_sem).start()
        for d in range(1, n_row):
            mp_copy(d).start()

    def global_row(t):
        return jnp.concatenate([as_row(window(t, chip * 2)), as_row(window(t, chip * 2 + 1))], axis=1)

    def global_col(t):
        return jnp.concatenate([window(t, chip * 2), window(t, chip * 2 + 1)], axis=0)

    def same_slots(t):
        row = global_row(t)
        return jnp.where((global_col(t - 1) == row) & (row >= 0.0), 1.0, 0.0).astype(BF)

    def energy(v):
        return jnp.sum(v * v, axis=0, keepdims=True)

    def prefetch(i, count):
        width = ahead // count
        for d in range(1, n_row):
            piece = pl.ds(i * width, width)
            put(a_vm.at[:, piece], a_peer.at[d - 1, :, piece], ap_sem, row_at(d), col)

    current = None
    energies = []
    for t in range(iters - 1):
        if t == 0:
            relay_kept(0)
            took(part_recv.at[pl.ds(0, 2 * n_row - 1)], part_sem)
            gradient = jnp.concatenate(
                [sum(part_recv[2 * d + b].astype(F32) for d in range(n_row)) for b in range(2)], axis=1
            )
            current = STEP_SIZE * gradient
            wait_kept(0)
        else:
            rows = [
                jnp.concatenate(
                    [
                        jnp.concatenate([res[t, g * gm + r * gr + j] for j in range(gr)], axis=1)
                        for g in range(gs)
                    ],
                    axis=0,
                )
                for r in range(n_row)
            ]
            gradient = sum(nt(rows[r], kept[t, r]) for r in range(n_row))
            hi, lo = split(current)
            moved = same_slots(t)
            current = nn(hi, moved) + nn(lo, moved) + STEP_SIZE * gradient
        rounded = current.astype(BF)
        for r in range(n_row):
            image = nn(rounded, kept[t, r]).astype(BF)
            for g in range(gs):
                for j in range(gr):
                    img[t, g * gm + r * gr + j] = image[g * ps:(g + 1) * ps, j * pm:(j + 1) * pm]
        for k in range(1, chips):
            put(img.at[t, chip_at(k)], rs.at[t, k - 1], rs_sem.at[t], x, chip_at(k) * 2 + core)
        if t == 0:
            place_onehot(1)
            gather_kept(1)
            send_kept(1)
            took(mpiece, mp_sem)
            energies.append(energy(mpiece[...]))
        took(rs.at[t], rs_sem.at[t])
        summed = img[t, chip].astype(F32) + sum(rs[t, k].astype(F32) for k in range(chips - 1))
        residual = mpiece[...] - summed
        energies.append(energy(residual))
        last = t == iters - 2
        if not last:
            res[t + 1, chip] = residual.astype(BF)
            for k in range(1, chips):
                piece = res.at[t + 1, chip]
                put(piece, piece, ag_sem.at[t], x, chip_at(k) * 2 + core)
            if t == 0:
                relay_kept(1)
                for u in range(2, iters - 1):
                    place_onehot(u)
                    gather_kept(u)
                    send_kept(u)
                if ahead:
                    for i in range(4):
                        prefetch(i, 4)
                wait_kept(1)
            if t == 1:
                for u in range(2, iters - 1):
                    relay_kept(u)
                    wait_kept(u)
            took(res.at[0, pl.ds(0, chips - 1)], ag_sem.at[t])
        else:
            fin[core, chip] = residual.astype(BF)

    last_piece = fin.at[core, chip]
    foth_from = counter[0]
    counter[0] += chips
    away = lax.rem(owner_row + n_row - x, n_row)
    slot = gi * gr + lax.rem(gj, gr)

    def foth_copy(k):
        return pltpu.make_async_remote_copy(
            src_ref=last_piece, dst_ref=foth.at[jnp.maximum(away - 1, 0), core, slot],
            send_sem=send.at[foth_from + k], recv_sem=foth_sem,
            device_id={"row": owner_row, "col": chip_at(k) * 2 + core}, device_id_type=MESH,
        )

    @pl.when(away > 0)
    def _():
        for k in range(chips):
            foth_copy(k).start()

    for k in range(1, chips):
        put(last_piece, last_piece, fin_sem, x, chip_at(k) * 2 + core)

    lanes = e_send.shape[2]
    folded = [sum(e[:, i * lanes:(i + 1) * lanes] for i in range(pm // lanes)) for e in energies]
    for t in range(iters):
        e_send[t] = folded[t]
    for d in range(n_row):
        for k in range(chips):
            if d or k:
                put(e_send, e_recv.at[d * chips + k - 1], e_sem.at[0], row_at(d), chip_at(k) * 2 + core)

    for b in range(2):
        cur_send[b] = current[:, b * KMAX:(b + 1) * KMAX]
    put(cur_send.at[other], cur_recv.at[core], core_sem.at[0], x, partner)
    cur_recv[core] = cur_send[core]

    keep = jnp.sum(jnp.where(marks(iters - 1), 1.0, 0.0), axis=0, keepdims=True)

    took(foth.at[:, 0], foth_sem)
    for d in range(1, n_row):
        got = foth.at[d - 1, core]
        put(got, got, core_sem.at[1 + d], x, partner)
    took(fin.at[0, pl.ds(0, chips - 1)], fin_sem)
    put(fin.at[core], fin.at[core], core_sem.at[1], x, partner)
    for d in range(1, n_row):
        took(foth.at[d - 1, 0], core_sem.at[1 + d])

    count = columns // CHUNK
    first = ahead // CHUNK
    for d in range(1, n_row):
        theirs = jnp.concatenate(
            [
                jnp.concatenate([foth[d - 1, c, g * gr + j] for j in range(gr)], axis=1)
                for c in range(2) for g in range(gs)
            ],
            axis=0,
        )
        for i in range(first, count):
            qsend[d - 1, i - first] = nn(theirs, a_vm[:, i * CHUNK:(i + 1) * CHUNK]).astype(BF)
            put(qsend.at[d - 1, i - first], qrecv.at[d - 1, i - first], q_sem.at[d - 1, i - first], row_from(d), col)

    took(fin.at[0], core_sem.at[1])
    took(cur_recv.at[0], core_sem.at[0])

    def residual_of(r):
        return jnp.concatenate(
            [
                jnp.concatenate([fin[c, g * gm + r * gr + j] for j in range(gr)], axis=1)
                for c in range(2) for g in range(gs)
            ],
            axis=0,
        )

    own = residual_of(x)
    last_hi, last_lo = split(jnp.concatenate([cur_recv[0], cur_recv[1]], axis=0))

    def finish(i, extra):
        at = slice(i * CHUNK, (i + 1) * CHUNK)
        marked = onehot[iters - 2, :, at]
        stepped = nn(last_hi, marked) + nn(last_lo, marked)
        stepped = stepped + STEP_SIZE * (nn(own, a_vm[:, at]) + extra)
        out_ref[:, at] = stepped * keep[:, at]
        nrm_send[i] = jnp.sum(stepped * stepped, axis=0, keepdims=True)

    if ahead:
        took(a_peer, ap_sem)
        peers = [residual_of(row_from(d)) for d in range(1, n_row)]
        for i in range(first):
            at = slice(i * CHUNK, (i + 1) * CHUNK)
            finish(i, sum(nn(peers[d - 1], a_peer[d - 1, :, at]) for d in range(1, n_row)))
        for d in range(1, n_row):
            piece = pl.ds(0, first)
            put(nrm_send.at[piece], nrm_recv.at[d - 1, piece], nrm_sem.at[0], row_at(d), col)

    took(e_recv, e_sem.at[0])
    total = e_send[...] + sum(e_recv[k] for k in range(n_row * chips - 1))
    e_both[0] = total
    put(e_both.at[0], e_both.at[1], e_sem.at[1], x, partner)

    for i in range(first, count):
        for d in range(1, n_row):
            took(qrecv.at[d - 1, i - first], q_sem.at[d - 1, i - first])
        finish(i, sum(qrecv[d - 1, i - first].astype(F32) for d in range(1, n_row)))
    for d in range(1, n_row):
        piece = pl.ds(first, count - first)
        put(nrm_send.at[piece], nrm_recv.at[d - 1, piece], nrm_sem.at[1], row_at(d), col)

    took(e_both.at[1], e_sem.at[1])
    en_ref[...] = e_both[0] + e_both[1]
    if ahead:
        took(nrm_recv.at[:, pl.ds(0, first)], nrm_sem.at[0])
    took(nrm_recv.at[:, pl.ds(first, count - first)], nrm_sem.at[1])
    sums_ref[...] = nrm_send[...] + sum(nrm_recv[d - 1] for d in range(1, n_row))

    drain()

    @pl.when(owner_row == x)
    def _():
        for d in range(1, n_row):
            mp_copy(d).wait_send()

    @pl.when(away > 0)
    def _():
        for k in range(chips):
            foth_copy(k).wait_send()


def local(matrix, measured, support):
    signals, mb = measured.shape
    columns = matrix.shape[1]
    iters = support.shape[0]
    n_row = lax.axis_size("row")
    n_col = lax.axis_size("col")
    s = sizes(n_row, n_col, signals, mb, columns, iters)
    chips, mine, ps, pm, gs, gr, half = (s[k] for k in ("chips", "mine", "ps", "pm", "gs", "gr", "half"))
    count = columns // CHUNK
    late = count - s["ahead"] // CHUNK
    peers = n_row - 1
    dma = pltpu.SemaphoreType.DMA
    vm = pltpu.VMEM
    outs = pl.pallas_call(
        functools.partial(kernel, s),
        out_shape=(
            jax.ShapeDtypeStruct((half, columns), F32),
            jax.ShapeDtypeStruct((count, 1, CHUNK), F32),
            jax.ShapeDtypeStruct((iters, 1, 128), F32),
        ),
        in_specs=[
            pl.BlockSpec(memory_space=vm),
            pl.BlockSpec(memory_space=pltpu.HBM),
            pl.BlockSpec(memory_space=pltpu.HBM),
        ],
        out_specs=(pl.BlockSpec(memory_space=vm),) * 3,
        scratch_shapes=[
            vm((mb, columns), BF),
            vm((signals, mb), F32),
            vm((ps, pm), F32),
            vm((iters - 1, KMAX, columns), BF),
            vm((iters - 1, n_row, 2 * KMAX, mb), BF),
            vm((n_row, 2, mine, KMAX), BF),
            vm((2 * n_row, mine, KMAX), BF),
            vm((iters - 1, chips, ps, pm), BF),
            vm((iters - 1, chips - 1, ps, pm), BF),
            vm((iters - 1, chips, ps, pm), BF),
            vm((2, chips, ps, pm), BF),
            vm((peers, 2, gs * gr, ps, pm), BF),
            vm((2, mine, KMAX), F32),
            vm((2, mine, KMAX), F32),
            vm((peers, late, half, CHUNK), BF),
            vm((peers, late, half, CHUNK), BF),
            vm((peers, mb, max(s["ahead"], 128)), BF),
            vm((count, 1, CHUNK), F32),
            vm((peers, count, 1, CHUNK), F32),
            vm((iters, 1, 128), F32),
            vm((n_row * chips - 1, iters, 1, 128), F32),
            vm((2, iters, 1, 128), F32),
            dma((4,)),
            dma,
            dma,
            dma((512 if n_row == 2 else 1024,)),
            dma((iters - 1, peers)),
            dma((iters - 1, n_row)),
            dma,
            dma((iters - 1,)),
            dma((iters - 1,)),
            dma,
            dma,
            dma((2 + n_row,)),
            dma((peers, late)),
            dma,
            dma((2,)),
            dma((2,)),
        ],
        compiler_params=pltpu.CompilerParams(
            collective_id=0, has_side_effects=True, vmem_limit_bytes=60 * 1024 * 1024
        ),
    )(support, measured, matrix)
    estimate, squares, energy = outs
    entries = signals * mb * n_row
    return (
        estimate,
        jnp.sqrt(squares.reshape(columns)),
        jnp.sum(energy, axis=(1, 2)) / entries,
    )


def solution(mesh):
    placed = (P("row", "col"), P(None, "row"), P())
    return jax.shard_map(
        local,
        mesh=mesh,
        in_specs=placed,
        out_specs=(P("row", "col"), P("col"), P()),
        check_vma=False,
    )
```

```python
import functools

import jax
import jax.numpy as jnp
from jax import lax
from jax.experimental import pallas as pl
from jax.experimental.pallas import tpu as pltpu
from jax.sharding import PartitionSpec as P

MESH = pl.DeviceIdType.MESH
KMAX = 128
STEP_SIZE = 0.25
CHUNK = 256
AHEAD = 1280
BF = jnp.bfloat16
F32 = jnp.float32
NT = (((1,), (1,)), ((), ()))


def nn(a, b):
    return jnp.dot(a, b, preferred_element_type=F32)


def nt(a, b):
    return lax.dot_general(a, b, NT, preferred_element_type=F32)


def split(v):
    hi = v.astype(BF)
    return hi, (v - hi.astype(F32)).astype(BF)


def sizes(n_row, n_col, signals, mb, columns, iterations):
    chips = n_col // 2
    mine = signals // n_row // 2
    groups = max(1, min(mine // 16, chips))
    parts = chips // groups
    total = mb * n_row
    return dict(
        n_row=n_row, chips=chips, mine=mine, gs=groups, gm=parts, ps=mine // groups, pm=total // parts,
        mb=mb, columns=columns, iters=iterations, half=signals // n_row, signals=signals,
        gr=parts // n_row, ahead=min(AHEAD, columns // 2) if n_row == 2 else 0,
    )


def kernel(
    s, supp_ref, meas_ref, a_ref, out_ref, sums_ref, en_ref,
    a_vm, mpiece, onehot, same, kept, part_send, part_recv, img, rs, res, fin, foth,
    cur_send, cur_recv, qsend, qrecv, a_peer, nrm_send, nrm_recv, e_send, e_recv, e_both,
    a_sem, mp_sem, mp_left, kept_left, part_left, rs_left, ag_left, fin_left, foth_left,
    q_left, ap_left, nrm_left, e_left, kept_recv, kept_core, part_sem, rs_sem, ag_sem, fin_sem, foth_sem,
    core_sem, q_sem, ap_sem, nrm_sem, e_sem,
):
    n_row, chips, mine, gs, gm, ps, pm = (s[k] for k in ("n_row", "chips", "mine", "gs", "gm", "ps", "pm"))
    mb, columns, iters, half, gr, ahead = (s[k] for k in ("mb", "columns", "iters", "half", "gr", "ahead"))
    x = lax.axis_index("row")
    col = lax.axis_index("col")
    chip = col // 2
    core = col % 2
    other = 1 - core
    sent = []

    def put(src, dst, left, recv, row, column):
        pltpu.make_async_remote_copy(
            src_ref=src, dst_ref=dst, send_sem=left, recv_sem=recv,
            device_id={"row": row, "col": column}, device_id_type=MESH,
        ).start()

    def took(ref, sem):
        pltpu.make_async_copy(ref, ref, sem).wait()

    def left_later(ref, sem):
        sent.append((ref, sem))

    def row_at(d):
        return lax.rem(x + d, n_row)

    def row_from(d):
        return lax.rem(x + n_row - d, n_row)

    def chip_at(k):
        return lax.rem(chip + k, chips)

    partner = chip * 2 + other

    strips = 4
    strip = mb // strips
    loads = [
        pltpu.make_async_copy(a_ref.at[pl.ds(i * strip, strip)], a_vm.at[pl.ds(i * strip, strip)], a_sem.at[i])
        for i in range(strips)
    ]
    for load in loads:
        load.start()

    barrier = pltpu.get_barrier_semaphore()
    greeted = 0
    for d in range(n_row):
        for k in range(chips):
            if d or k:
                pl.semaphore_signal(
                    barrier, inc=1, device_id={"row": row_at(d), "col": chip_at(k) * 2 + core}, device_id_type=MESH
                )
                greeted += 1
        pl.semaphore_signal(barrier, inc=1, device_id={"row": row_at(d), "col": partner}, device_id_type=MESH)
        greeted += 1

    k_all = supp_ref.shape[1]
    lane_k = lax.broadcasted_iota(jnp.int32, (1, k_all), 1).astype(F32)
    slot_k = lax.broadcasted_iota(jnp.int32, (KMAX, k_all), 0).astype(F32)
    eye = lax.broadcasted_iota(jnp.int32, (KMAX, KMAX), 0) == lax.broadcasted_iota(jnp.int32, (KMAX, KMAX), 1)
    lane_n = lax.broadcasted_iota(jnp.int32, (1, columns), 1).astype(F32)

    def window(t, block):
        row = supp_ref[pl.ds(t, 1), :].astype(F32)
        start = (block * columns).astype(F32)
        below = jnp.sum((row < start).astype(F32), axis=1, keepdims=True)
        inside = (row >= start) & (row < start + columns)
        chosen = ((lane_k - below) == slot_k) & inside
        return jnp.sum(jnp.where(chosen, row + 1.0, 0.0), axis=1, keepdims=True) - 1.0

    def as_row(index):
        return jnp.sum(jnp.where(eye, index, 0.0), axis=0, keepdims=True)

    def marks(t):
        return (window(t, col) - (col * columns).astype(F32)) == lane_n

    def place_onehot(t):
        onehot[t] = jnp.where(marks(t), 1.0, 0.0).astype(BF)

    my_slots = pl.ds(pl.multiple_of(core * KMAX, KMAX), KMAX)

    def gather_kept(t):
        if t == 0:
            for load in loads:
                load.wait()
        for i in range(strips):
            picked = nt(onehot[t], a_vm[i * strip:(i + 1) * strip, :])
            kept[t, x, my_slots, i * strip:(i + 1) * strip] = picked.astype(BF)

    def send_kept(t):
        mine_kept = kept.at[t, x, my_slots]
        put(mine_kept, mine_kept, kept_left.at[t, 0], kept_core.at[t, 0], x, partner)
        for d in range(1, n_row):
            put(mine_kept, mine_kept, kept_left.at[t, 1], kept_recv.at[t, d - 1], row_at(d), col)
        pieces = kept.at[t, pl.ds(0, n_row - 1), pl.ds(0, KMAX)]
        left_later(kept.at[t, 0, pl.ds(0, KMAX)], kept_left.at[t, 0])
        left_later(pieces, kept_left.at[t, 1])
        left_later(pieces, kept_left.at[t, 2])

    def relay_kept(t):
        for d in range(1, n_row):
            got = kept.at[t, row_from(d), my_slots]
            took(got, kept_recv.at[t, d - 1])
            put(got, got, kept_left.at[t, 2], kept_core.at[t, d], x, partner)

    def wait_kept(t):
        for d in range(n_row):
            took(kept.at[t, 0, pl.ds(0, KMAX)], kept_core.at[t, d])

    place_onehot(0)
    gather_kept(0)
    pl.semaphore_wait(barrier, greeted)
    send_kept(0)

    kept_mine = kept[0, x, my_slots, :]
    part = nt(meas_ref[...].astype(BF), kept_mine).astype(BF)
    for r in range(n_row):
        for c in range(2):
            base = r * half + c * mine
            part_send[r, c] = part[base:base + mine]
    for d in range(n_row):
        if d:
            put(part_send.at[row_at(d), core], part_recv.at[2 * d + core], part_left, part_sem, row_at(d), col)
        put(part_send.at[row_at(d), other], part_recv.at[2 * d + core], part_left, part_sem, row_at(d), partner)
    left_later(part_recv.at[pl.ds(0, 2 * n_row - 1)], part_left)
    part_recv[core] = part_send[x, core]

    gi = chip // gm
    gj = lax.rem(chip, gm)
    owner_row = gj // gr
    piece_lane = pl.ds(pl.multiple_of(lax.rem(gj, gr) * pm, 128), pm)

    def piece_rows(r):
        return pl.ds(pl.multiple_of(r * half + core * mine + gi * ps, 8), ps)

    def mp_copy(d):
        return pltpu.make_async_remote_copy(
            src_ref=meas_ref.at[piece_rows(row_at(d)), piece_lane], dst_ref=mpiece,
            send_sem=mp_left.at[d - 1], recv_sem=mp_sem,
            device_id={"row": row_at(d), "col": col}, device_id_type=MESH,
        )

    @pl.when(owner_row == x)
    def _():
        mpiece[...] = meas_ref[piece_rows(x), piece_lane]
        for d in range(1, n_row):
            mp_copy(d).start()

    for t in range(1, iters - 1):
        place_onehot(t)
        gather_kept(t)
        send_kept(t)

    def global_row(t):
        return jnp.concatenate([as_row(window(t, chip * 2)), as_row(window(t, chip * 2 + 1))], axis=1)

    def global_col(t):
        return jnp.concatenate([window(t, chip * 2), window(t, chip * 2 + 1)], axis=0)

    def same_slots(t):
        row = global_row(t)
        return jnp.where((global_col(t - 1) == row) & (row >= 0.0), 1.0, 0.0).astype(BF)

    def energy(v):
        return jnp.sum(v * v, axis=0, keepdims=True)

    count = columns // CHUNK
    first = ahead // CHUNK

    def prefetch(i):
        for d in range(1, n_row):
            piece = pl.ds(i * CHUNK, CHUNK)
            put(a_vm.at[:, piece], a_peer.at[d - 1, :, piece], ap_left, ap_sem, row_at(d), col)

    current = None
    energies = []
    for t in range(iters - 1):
        if t == 0:
            relay_kept(0)
            took(part_recv.at[pl.ds(0, 2 * n_row - 1)], part_sem)
            gradient = jnp.concatenate(
                [sum(part_recv[2 * d + b].astype(F32) for d in range(n_row)) for b in range(2)], axis=1
            )
            current = STEP_SIZE * gradient
            wait_kept(0)
        else:
            rows = [
                jnp.concatenate(
                    [
                        jnp.concatenate([res[t, g * gm + r * gr + j] for j in range(gr)], axis=1)
                        for g in range(gs)
                    ],
                    axis=0,
                )
                for r in range(n_row)
            ]
            gradient = sum(nt(rows[r], kept[t, r]) for r in range(n_row))
            hi, lo = split(current)
            moved = same[t]
            current = nn(hi, moved) + nn(lo, moved) + STEP_SIZE * gradient
        rounded = current.astype(BF)
        for r in range(n_row):
            image = nn(rounded, kept[t, r]).astype(BF)
            for g in range(gs):
                for j in range(gr):
                    img[t, g * gm + r * gr + j] = image[g * ps:(g + 1) * ps, j * pm:(j + 1) * pm]
        for k in range(1, chips):
            put(img.at[t, chip_at(k)], rs.at[t, k - 1], rs_left.at[t], rs_sem.at[t], x, chip_at(k) * 2 + core)
        left_later(rs.at[t], rs_left.at[t])
        if t == 0:
            for i in range(first - 1):
                prefetch(i)

            @pl.when(owner_row != x)
            def _():
                took(mpiece, mp_sem)

            energies.append(energy(mpiece[...]))
            for u in range(1, iters - 1):
                same[u] = same_slots(u)
            keep = jnp.sum(jnp.where(marks(iters - 1), 1.0, 0.0), axis=0, keepdims=True)
            relay_kept(1)
        took(rs.at[t], rs_sem.at[t])
        summed = img[t, chip].astype(F32) + sum(rs[t, k].astype(F32) for k in range(chips - 1))
        residual = mpiece[...] - summed
        energies.append(energy(residual))
        last = t == iters - 2
        if not last:
            res[t + 1, chip] = residual.astype(BF)
            for k in range(1, chips):
                piece = res.at[t + 1, chip]
                put(piece, piece, ag_left.at[t], ag_sem.at[t], x, chip_at(k) * 2 + core)
            left_later(res.at[0, pl.ds(0, chips - 1)], ag_left.at[t])
            if t == 0:
                for u in range(2, iters - 1):
                    relay_kept(u)
            wait_kept(t + 1)
            took(res.at[0, pl.ds(0, chips - 1)], ag_sem.at[t])
        else:
            fin[core, chip] = residual.astype(BF)

    last_piece = fin.at[core, chip]
    away = lax.rem(owner_row + n_row - x, n_row)
    slot = gi * gr + lax.rem(gj, gr)

    def foth_copy(k):
        return pltpu.make_async_remote_copy(
            src_ref=last_piece, dst_ref=foth.at[jnp.maximum(away - 1, 0), core, slot],
            send_sem=foth_left, recv_sem=foth_sem,
            device_id={"row": owner_row, "col": chip_at(k) * 2 + core}, device_id_type=MESH,
        )

    @pl.when(away > 0)
    def _():
        for k in range(chips):
            foth_copy(k).start()

    if first:
        prefetch(first - 1)
    for k in range(1, chips):
        put(last_piece, last_piece, fin_left.at[0], fin_sem, x, chip_at(k) * 2 + core)

    left_later(fin.at[0, pl.ds(0, chips - 1)], fin_left.at[0])

    lanes = e_send.shape[2]
    folded = [sum(e[:, i * lanes:(i + 1) * lanes] for i in range(pm // lanes)) for e in energies]
    for t in range(iters):
        e_send[t] = folded[t]
    for d in range(n_row):
        for k in range(chips):
            if d or k:
                put(e_send, e_recv.at[d * chips + k - 1], e_left.at[0], e_sem.at[0], row_at(d), chip_at(k) * 2 + core)

    left_later(e_recv, e_left.at[0])

    for b in range(2):
        cur_send[b] = current[:, b * KMAX:(b + 1) * KMAX]
    put(cur_send.at[other], cur_recv.at[core], fin_left.at[1], core_sem.at[0], x, partner)
    left_later(cur_recv.at[0], fin_left.at[1])
    cur_recv[core] = cur_send[core]

    took(foth.at[:, 0], foth_sem)
    for d in range(1, n_row):
        got = foth.at[d - 1, core]
        put(got, got, fin_left.at[2], core_sem.at[1 + d], x, partner)
    took(fin.at[0, pl.ds(0, chips - 1)], fin_sem)
    put(fin.at[core], fin.at[core], fin_left.at[3], core_sem.at[1], x, partner)
    left_later(foth.at[:, 0], fin_left.at[2])
    left_later(fin.at[0], fin_left.at[3])
    for d in range(1, n_row):
        took(foth.at[d - 1, 0], core_sem.at[1 + d])

    for d in range(1, n_row):
        theirs = jnp.concatenate(
            [
                jnp.concatenate([foth[d - 1, c, g * gr + j] for j in range(gr)], axis=1)
                for c in range(2) for g in range(gs)
            ],
            axis=0,
        )
        for i in range(first, count):
            qsend[d - 1, i - first] = nn(theirs, a_vm[:, i * CHUNK:(i + 1) * CHUNK]).astype(BF)
            put(
                qsend.at[d - 1, i - first], qrecv.at[d - 1, i - first], q_left, q_sem.at[d - 1, i - first],
                row_from(d), col,
            )

    left_later(qsend, q_left)

    took(fin.at[0], core_sem.at[1])
    took(cur_recv.at[0], core_sem.at[0])

    def residual_of(r):
        return jnp.concatenate(
            [
                jnp.concatenate([fin[c, g * gm + r * gr + j] for j in range(gr)], axis=1)
                for c in range(2) for g in range(gs)
            ],
            axis=0,
        )

    own = residual_of(x)
    last_hi, last_lo = split(jnp.concatenate([cur_recv[0], cur_recv[1]], axis=0))

    lines = CHUNK // 128

    def finish(i, extra):
        at = slice(i * CHUNK, (i + 1) * CHUNK)
        marked = onehot[iters - 2, :, at]
        stepped = nn(last_hi, marked) + nn(last_lo, marked)
        stepped = stepped + STEP_SIZE * (nn(own, a_vm[:, at]) + extra)
        out_ref[:, at] = stepped * keep[:, at]
        squares = jnp.sum(stepped * stepped, axis=0, keepdims=True)
        for j in range(lines):
            nrm_send[i, j:j + 1] = squares[:, j * 128:(j + 1) * 128]

    if ahead:
        took(a_peer, ap_sem)
        peers = [residual_of(row_from(d)) for d in range(1, n_row)]
        for i in range(first):
            at = slice(i * CHUNK, (i + 1) * CHUNK)
            finish(i, sum(nn(peers[d - 1], a_peer[d - 1, :, at]) for d in range(1, n_row)))
        for d in range(1, n_row):
            piece = pl.ds(0, first)
            put(nrm_send.at[piece], nrm_recv.at[d - 1, piece], nrm_left.at[0], nrm_sem.at[0], row_at(d), col)

        left_later(nrm_recv.at[:, pl.ds(0, first)], nrm_left.at[0])
        left_later(a_peer, ap_left)

    took(e_recv, e_sem.at[0])
    total = e_send[...] + sum(e_recv[k] for k in range(n_row * chips - 1))
    e_both[0] = total
    put(e_both.at[0], e_both.at[1], e_left.at[1], e_sem.at[1], x, partner)
    left_later(e_both.at[0], e_left.at[1])

    for i in range(first, count):
        for d in range(1, n_row):
            took(qrecv.at[d - 1, i - first], q_sem.at[d - 1, i - first])
        finish(i, sum(qrecv[d - 1, i - first].astype(F32) for d in range(1, n_row)))
    for d in range(1, n_row):
        piece = pl.ds(first, count - first)
        put(nrm_send.at[piece], nrm_recv.at[d - 1, piece], nrm_left.at[1], nrm_sem.at[1], row_at(d), col)
    left_later(nrm_recv.at[:, pl.ds(first, count - first)], nrm_left.at[1])

    took(e_both.at[1], e_sem.at[1])
    entries = s["signals"] * mb * n_row
    for t in range(iters):
        en_ref[t] = jnp.sum(e_both[0, t] + e_both[1, t]) / entries
    if ahead:
        took(nrm_recv.at[:, pl.ds(0, first)], nrm_sem.at[0])
    took(nrm_recv.at[:, pl.ds(first, count - first)], nrm_sem.at[1])
    for i in range(count):
        squares = nrm_send[i] + sum(nrm_recv[d - 1, i] for d in range(1, n_row))
        sums_ref[i * lines:(i + 1) * lines] = jnp.sqrt(squares)

    for ref, sem in sent:
        took(ref, sem)

    @pl.when(owner_row == x)
    def _():
        for d in range(1, n_row):
            mp_copy(d).wait_send()

    @pl.when(away > 0)
    def _():
        took(fin.at[0], foth_left)


def local(matrix, measured, support):
    signals, mb = measured.shape
    columns = matrix.shape[1]
    iters = support.shape[0]
    n_row = lax.axis_size("row")
    n_col = lax.axis_size("col")
    s = sizes(n_row, n_col, signals, mb, columns, iters)
    chips, mine, ps, pm, gs, gr, half = (s[k] for k in ("chips", "mine", "ps", "pm", "gs", "gr", "half"))
    count = columns // CHUNK
    late = count - s["ahead"] // CHUNK
    peers = n_row - 1
    dma = pltpu.SemaphoreType.DMA
    vm = pltpu.VMEM
    outs = pl.pallas_call(
        functools.partial(kernel, s),
        out_shape=(
            jax.ShapeDtypeStruct((half, columns), F32),
            jax.ShapeDtypeStruct((columns // 128, 128), F32),
            jax.ShapeDtypeStruct((iters,), F32),
        ),
        in_specs=[
            pl.BlockSpec(memory_space=vm),
            pl.BlockSpec(memory_space=vm),
            pl.BlockSpec(memory_space=pltpu.HBM),
        ],
        out_specs=(
            pl.BlockSpec(memory_space=vm), pl.BlockSpec(memory_space=vm), pl.BlockSpec(memory_space=pltpu.SMEM)
        ),
        scratch_shapes=[
            vm((mb, columns), BF),
            vm((ps, pm), F32),
            vm((iters - 1, KMAX, columns), BF),
            vm((iters - 1, 2 * KMAX, 2 * KMAX), BF),
            vm((iters - 1, n_row, 2 * KMAX, mb), BF),
            vm((n_row, 2, mine, KMAX), BF),
            vm((2 * n_row, mine, KMAX), BF),
            vm((iters - 1, chips, ps, pm), BF),
            vm((iters - 1, chips - 1, ps, pm), BF),
            vm((iters - 1, chips, ps, pm), BF),
            vm((2, chips, ps, pm), BF),
            vm((peers, 2, gs * gr, ps, pm), BF),
            vm((2, mine, KMAX), F32),
            vm((2, mine, KMAX), F32),
            vm((peers, late, half, CHUNK), BF),
            vm((peers, late, half, CHUNK), BF),
            vm((peers, mb, max(s["ahead"], 128)), BF),
            vm((count, CHUNK // 128, 128), F32),
            vm((peers, count, CHUNK // 128, 128), F32),
            vm((iters, 1, 128), F32),
            vm((n_row * chips - 1, iters, 1, 128), F32),
            vm((2, iters, 1, 128), F32),
            dma((4,)),
            dma,
            dma((peers,)),
            dma((iters - 1, 3)),
            dma,
            dma((iters - 1,)),
            dma((iters - 1,)),
            dma((4,)),
            dma,
            dma,
            dma,
            dma((2,)),
            dma((2,)),
            dma((iters - 1, peers)),
            dma((iters - 1, n_row)),
            dma,
            dma((iters - 1,)),
            dma((iters - 1,)),
            dma,
            dma,
            dma((2 + n_row,)),
            dma((peers, late)),
            dma,
            dma((2,)),
            dma((2,)),
        ],
        compiler_params=pltpu.CompilerParams(
            collective_id=0, has_side_effects=True, vmem_limit_bytes=50 * 1024 * 1024
        ),
    )(support, measured, matrix)
    estimate, norms, energy = outs
    return estimate, norms.reshape(columns), energy


def solution(mesh):
    placed = (P("row", "col"), P(None, "row"), P())
    return jax.shard_map(
        local,
        mesh=mesh,
        in_specs=placed,
        out_specs=(P("row", "col"), P("col"), P()),
        check_vma=False,
    )
```

```python
import functools

import jax
import jax.numpy as jnp
from jax import lax
from jax.experimental import pallas as pl
from jax.experimental.pallas import tpu as pltpu
from jax.sharding import PartitionSpec as P

MESH = pl.DeviceIdType.MESH
KMAX = 128
STEP_SIZE = 0.25
CHUNK = 256
AHEAD = 896
LATE = 1
BF = jnp.bfloat16
F32 = jnp.float32
NT = (((1,), (1,)), ((), ()))


def nn(a, b):
    return jnp.dot(a, b, preferred_element_type=F32)


def nt(a, b):
    return lax.dot_general(a, b, NT, preferred_element_type=F32)


def split(v):
    hi = v.astype(BF)
    return hi, (v - hi.astype(F32)).astype(BF)


def sizes(n_row, n_col, signals, mb, columns, iterations):
    chips = n_col // 2
    mine = signals // n_row // 2
    chains = 2 if mine % 32 == 0 else 1
    sub = mine // chains
    groups = max(1, min(sub // 16, chips))
    parts = chips // groups
    total = mb * n_row
    return dict(
        n_row=n_row, chips=chips, mine=mine, chains=chains, sub=sub, gs=groups, gm=parts,
        ps=sub // groups, pm=total // parts, mb=mb, columns=columns, iters=iterations,
        half=signals // n_row, signals=signals, gr=parts // n_row,
        ahead=min(AHEAD, columns // 2) if n_row == 2 else 0,
    )


def cut(start, stop):
    edges = list(range(start, stop, CHUNK)) + [stop]
    if edges[-1] - edges[-2] > 128:
        edges.insert(-1, edges[-1] - 128)
    return [slice(a, b) for a, b in zip(edges[:-1], edges[1:])]


def kernel(
    s, supp_hbm, meas_hbm, a_ref, out_ref, sums_ref,
    a_vm, supp_ref, meas_ref, mpiece, onehot, same, kept, part_send, part_recv, img, rs, first_out, res, fin, foth,
    cur_send, cur_recv, qsend, qrecv, a_peer, nrm_send, nrm_recv, e_send, e_recv, e_both,
    in_sem, a_sem, mp_sem, mp_left, kept_left, part_left, rs_left, ag_left, first_left, fin_left, fin_core_left,
    foth_left, foth_core_left, cur_left, q_left, ap_left, nrm_left, e_left,
    kept_recv, kept_core, part_sem, rs_sem, ag_sem, fin_sem, fin_core, foth_sem, foth_core,
    cur_sem, q_sem, ap_sem, nrm_sem, e_sem,
):
    n_row, chips, mine, gs, gm, ps, pm = (s[k] for k in ("n_row", "chips", "mine", "gs", "gm", "ps", "pm"))
    chains, sub = s["chains"], s["sub"]
    mb, columns, iters, half, gr, ahead = (s[k] for k in ("mb", "columns", "iters", "half", "gr", "ahead"))
    x = lax.axis_index("row")
    col = lax.axis_index("col")
    chip = col // 2
    core = col % 2
    other = 1 - core
    sent = []

    def put(src, dst, left, recv, row, column):
        pltpu.make_async_remote_copy(
            src_ref=src, dst_ref=dst, send_sem=left, recv_sem=recv,
            device_id={"row": row, "col": column}, device_id_type=MESH,
        ).start()

    def took(ref, sem):
        pltpu.make_async_copy(ref, ref, sem).wait()

    def left_later(ref, sem):
        sent.append((ref, sem))

    def row_at(d):
        return lax.rem(x + d, n_row)

    def row_from(d):
        return lax.rem(x + n_row - d, n_row)

    def chip_at(k):
        return lax.rem(chip + k, chips)

    partner = chip * 2 + other

    supp_load = pltpu.make_async_copy(supp_hbm, supp_ref, in_sem.at[0])
    supp_load.start()
    strips = 4
    strip = mb // strips
    loads = [
        pltpu.make_async_copy(a_ref.at[pl.ds(i * strip, strip)], a_vm.at[pl.ds(i * strip, strip)], a_sem.at[i])
        for i in range(strips)
    ]
    for load in loads:
        load.start()

    meas_load = pltpu.make_async_copy(meas_hbm, meas_ref, in_sem.at[1])
    meas_load.start()

    barrier = pltpu.get_barrier_semaphore()
    greeted = 0
    for d in range(n_row):
        for k in range(chips):
            if d or k:
                pl.semaphore_signal(
                    barrier, inc=1, device_id={"row": row_at(d), "col": chip_at(k) * 2 + core}, device_id_type=MESH
                )
                greeted += 1
        pl.semaphore_signal(barrier, inc=1, device_id={"row": row_at(d), "col": partner}, device_id_type=MESH)
        greeted += 1

    k_all = supp_ref.shape[1]
    lane_k = lax.broadcasted_iota(jnp.int32, (1, k_all), 1).astype(F32)
    slot_k = lax.broadcasted_iota(jnp.int32, (KMAX, k_all), 0).astype(F32)
    eye = lax.broadcasted_iota(jnp.int32, (KMAX, KMAX), 0) == lax.broadcasted_iota(jnp.int32, (KMAX, KMAX), 1)
    lane_n = lax.broadcasted_iota(jnp.int32, (1, columns), 1).astype(F32)

    def window(t, block):
        row = supp_ref[pl.ds(t, 1), :].astype(F32)
        start = (block * columns).astype(F32)
        below = jnp.sum((row < start).astype(F32), axis=1, keepdims=True)
        inside = (row >= start) & (row < start + columns)
        chosen = ((lane_k - below) == slot_k) & inside
        return jnp.sum(jnp.where(chosen, row + 1.0, 0.0), axis=1, keepdims=True) - 1.0

    def as_row(index):
        return jnp.sum(jnp.where(eye, index, 0.0), axis=0, keepdims=True)

    def marks(t):
        return (window(t, col) - (col * columns).astype(F32)) == lane_n

    def place_onehot(t):
        onehot[t] = jnp.where(marks(t), 1.0, 0.0).astype(BF)

    my_slots = pl.ds(pl.multiple_of(core * KMAX, KMAX), KMAX)

    def gather_kept(t):
        if t == 0:
            for load in loads:
                load.wait()
        for i in range(0, mb, 128):
            picked = nt(onehot[t], a_vm[i:i + 128, :])
            kept[t, x, my_slots, i:i + 128] = picked.astype(BF)

    def send_kept(t):
        mine_kept = kept.at[t, x, my_slots]
        put(mine_kept, mine_kept, kept_left.at[t, 0], kept_core.at[t, 0], x, partner)
        left_later(kept.at[t, 0, pl.ds(0, KMAX)], kept_left.at[t, 0])
        if t:
            for d in range(1, n_row):
                put(mine_kept, mine_kept, kept_left.at[t, 1], kept_recv.at[t, d - 1], row_at(d), col)
            pieces = kept.at[t, pl.ds(0, n_row - 1), pl.ds(0, KMAX)]
            left_later(pieces, kept_left.at[t, 1])
            left_later(pieces, kept_left.at[t, 2])

    def relay_kept(t):
        for d in range(1, n_row):
            got = kept.at[t, row_from(d), my_slots]
            took(got, kept_recv.at[t, d - 1])
            put(got, got, kept_left.at[t, 2], kept_core.at[t, d], x, partner)

    def wait_kept(t):
        for d in range(n_row if t else 1):
            took(kept.at[t, 0, pl.ds(0, KMAX)], kept_core.at[t, d])

    supp_load.wait()
    place_onehot(0)
    gather_kept(0)
    pl.semaphore_wait(barrier, greeted)
    send_kept(0)

    meas_load.wait()
    kept_mine = kept[0, x, my_slots, :]
    part = nt(meas_ref[...].astype(BF), kept_mine).astype(BF)
    for r in range(n_row):
        for c in range(2):
            base = r * half + c * mine
            part_send[c, r] = part[base:base + mine]
    for d in range(n_row):
        if d:
            put(part_send.at[core], part_recv.at[2 * d + core], part_left, part_sem, row_at(d), col)
        put(part_send.at[other], part_recv.at[2 * d + core], part_left, part_sem, row_at(d), partner)
    left_later(part_recv.at[pl.ds(0, 2 * n_row - 1)], part_left)
    part_recv[core] = part_send[core]

    gi = chip // gm
    gj = lax.rem(chip, gm)
    owner_row = gj // gr
    piece_lane = pl.ds(pl.multiple_of(lax.rem(gj, gr) * pm, 128), pm)

    def piece_rows(r, h):
        return pl.ds(pl.multiple_of(r * half + core * mine + h * sub + gi * ps, 8), ps)

    def mp_copy(d, h):
        return pltpu.make_async_remote_copy(
            src_ref=meas_ref.at[piece_rows(row_at(d), h), piece_lane], dst_ref=mpiece.at[h],
            send_sem=mp_left.at[d - 1, h], recv_sem=mp_sem.at[h],
            device_id={"row": row_at(d), "col": col}, device_id_type=MESH,
        )

    @pl.when(owner_row == x)
    def _():
        for h in range(chains):
            mpiece[h] = meas_ref[piece_rows(x, h), piece_lane]
            for d in range(1, n_row):
                mp_copy(d, h).start()

    place_onehot(1)
    gather_kept(1)
    send_kept(1)

    def global_row(t):
        return jnp.concatenate([as_row(window(t, chip * 2)), as_row(window(t, chip * 2 + 1))], axis=1)

    def global_col(t):
        return jnp.concatenate([window(t, chip * 2), window(t, chip * 2 + 1)], axis=0)

    def same_slots(t):
        row = global_row(t)
        return jnp.where((global_col(t - 1) == row) & (row >= 0.0), 1.0, 0.0).astype(BF)

    def energy(v):
        return jnp.sum(v * v, axis=0, keepdims=True)

    lines = columns // 128
    near = ahead // 128
    early = max(near - LATE, 0)

    def prefetch(i):
        for d in range(1, n_row):
            piece = pl.ds(i * 128, 128)
            put(a_vm.at[:, piece], a_peer.at[d - 1, :, piece], ap_left, ap_sem, row_at(d), col)

    turn = chip // n_row
    to_row = lax.rem(chip + core, n_row)
    first_group = turn // gr
    first_part = lax.rem(turn, gr)
    first_slot = first_group * gm + x * gr + first_part
    first_lane = pl.ds(pl.multiple_of(first_part * pm, 128), pm)

    def first_copy(h):
        return pltpu.make_async_remote_copy(
            src_ref=first_out.at[h], dst_ref=res.at[1, h, first_slot],
            send_sem=first_left.at[h], recv_sem=ag_sem.at[0, h],
            device_id={"row": to_row, "col": col}, device_id_type=MESH,
        )

    def sum_of(t, h):
        took(rs.at[t, h], rs_sem.at[t, h])
        return img[t, h, chip].astype(F32) + sum(rs[t, h, k].astype(F32) for k in range(chips - 1))

    def scatter(t, h):
        for k in range(1, chips):
            put(
                img.at[t, h, chip_at(k)], rs.at[t, h, k - 1], rs_left.at[t, h], rs_sem.at[t, h],
                x, chip_at(k) * 2 + core,
            )
        left_later(rs.at[t, h], rs_left.at[t, h])

    def joined(buffer, r, blocks):
        return jnp.concatenate(
            [
                jnp.concatenate([buffer[b + (g * gm + r * gr + j,)] for j in range(gr)], axis=1)
                for b in blocks for g in range(gs)
            ],
            axis=0,
        )

    took(part_recv.at[pl.ds(0, 2 * n_row - 1)], part_sem)

    def first_step(rows):
        return STEP_SIZE * jnp.concatenate(
            [sum(part_recv[(2 * d + b,) + rows].astype(F32) for d in range(n_row)) for b in range(2)], axis=-1
        )

    wait_kept(0)
    for h in range(chains):
        at = slice(h * sub, (h + 1) * sub)
        rounded = jnp.concatenate([first_step((r, at)) for r in range(n_row)], axis=0).astype(BF)
        image = nn(rounded, kept[0, x]).astype(BF)
        for r in range(n_row):
            for g in range(gs):
                for j in range(gr):
                    place = (g * gr + j) * n_row + lax.rem(r + n_row - lax.rem(core, n_row), n_row)
                    img[0, h, place] = image[
                        r * sub + g * ps:r * sub + (g + 1) * ps, j * pm:(j + 1) * pm
                    ]
        scatter(0, h)
    for t in range(2, iters - 1):
        place_onehot(t)
        gather_kept(t)
        send_kept(t)
    mine_step = first_step((x,))
    current = [mine_step[h * sub:(h + 1) * sub] for h in range(chains)]

    @pl.when(owner_row != x)
    def _():
        for h in range(chains):
            took(mpiece.at[h], mp_sem.at[h])

    energies = [[energy(mpiece[h]) for h in range(chains)]]
    for u in range(1, iters - 1):
        same[u] = same_slots(u)
    keep = jnp.sum(jnp.where(marks(iters - 1), 1.0, 0.0), axis=0, keepdims=True)

    found = []
    for h in range(chains):
        rows = pl.ds(pl.multiple_of(to_row * half + core * mine + h * sub + first_group * ps, 8), ps)
        residual = meas_ref[rows, first_lane] - sum_of(0, h)
        found.append(energy(residual))
        first_out[h] = residual.astype(BF)
        for k in range(1, chips):
            put(
                first_out.at[h], res.at[1, h, first_slot], ag_left.at[0, h], ag_sem.at[0, h],
                to_row, chip_at(k) * 2 + core,
            )
        left_later(rs.at[0, 0], ag_left.at[0, h])

        @pl.when(to_row == x)
        def _():
            res[1, h, first_slot] = first_out[h]

        @pl.when(to_row != x)
        def _():
            first_copy(h).start()

    energies.append(found)
    relay_kept(1)
    for i in range(early):
        prefetch(i)
    wait_kept(1)

    away = lax.rem(owner_row + n_row - x, n_row)
    slot = gi * gr + lax.rem(gj, gr)

    def foth_copy(h, k):
        return pltpu.make_async_remote_copy(
            src_ref=fin.at[core, h, chip], dst_ref=foth.at[jnp.maximum(away - 1, 0), core, h, slot],
            send_sem=foth_left.at[h], recv_sem=foth_sem.at[h],
            device_id={"row": owner_row, "col": chip_at(k) * 2 + core}, device_id_type=MESH,
        )

    for t in range(1, iters - 1):
        carried = []
        for h in range(chains):
            hi, lo = split(current[h])
            carried.append(nn(hi, same[t]) + nn(lo, same[t]))
        for h in range(chains):
            if t == 1:

                @pl.when(to_row == x)
                def _():
                    took(res.at[1, h, pl.ds(0, chips - 1)], ag_sem.at[0, h])

                @pl.when(to_row != x)
                def _():
                    took(res.at[1, h], ag_sem.at[0, h])

            else:
                took(res.at[1, h, pl.ds(0, chips - 1)], ag_sem.at[t - 1, h])
            gradient = sum(nt(joined(res, r, [(t, h)]), kept[t, r]) for r in range(n_row))
            current[h] = carried[h] + STEP_SIZE * gradient
            rounded = current[h].astype(BF)
            for r in range(n_row):
                image = nn(rounded, kept[t, r]).astype(BF)
                for g in range(gs):
                    for j in range(gr):
                        img[t, h, g * gm + r * gr + j] = image[g * ps:(g + 1) * ps, j * pm:(j + 1) * pm]
            scatter(t, h)
        if t + 1 < iters - 1:
            relay_kept(t + 1)
            wait_kept(t + 1)
        found = []
        for h in range(chains):
            residual = mpiece[h] - sum_of(t, h)
            found.append(energy(residual))
            if t < iters - 2:
                res[t + 1, h, chip] = residual.astype(BF)
                piece = res.at[t + 1, h, chip]
                for k in range(1, chips):
                    put(piece, piece, ag_left.at[t, h], ag_sem.at[t, h], x, chip_at(k) * 2 + core)
                left_later(rs.at[0, 0], ag_left.at[t, h])
                continue
            fin[core, h, chip] = residual.astype(BF)

            @pl.when(away > 0)
            def _():
                for k in range(chips):
                    foth_copy(h, k).start()

            if h == chains - 1:
                for i in range(early, near):
                    prefetch(i)
            piece = fin.at[core, h, chip]
            for k in range(1, chips):
                put(piece, piece, fin_left.at[h], fin_sem.at[h], x, chip_at(k) * 2 + core)
            left_later(rs.at[0, 0], fin_left.at[h])
        energies.append(found)

    lanes = e_send.shape[2]
    folded = [
        sum(e[:, i * lanes:(i + 1) * lanes] for e in found for i in range(pm // lanes)) for found in energies
    ]
    for t in range(iters):
        e_send[t] = folded[t]
    for d in range(n_row):
        for k in range(chips):
            if d or k:
                put(e_send, e_recv.at[d * chips + k - 1], e_left.at[0], e_sem.at[0], row_at(d), chip_at(k) * 2 + core)

    left_later(e_recv, e_left.at[0])

    for b in range(2):
        for h in range(chains):
            cur_send[b, h * sub:(h + 1) * sub] = current[h][:, b * KMAX:(b + 1) * KMAX]
    put(cur_send.at[other], cur_recv.at[core], cur_left, cur_sem, x, partner)
    left_later(cur_recv.at[0], cur_left)
    cur_recv[core] = cur_send[core]

    spans = cut(ahead, columns)
    blocks = [(c, h) for c in range(2) for h in range(chains)]

    def relay_foth():
        for h in range(chains):
            took(foth.at[:, 0, h], foth_sem.at[h])
            for d in range(1, n_row):
                got = foth.at[d - 1, core, h]
                put(got, got, foth_core_left.at[h], foth_core.at[h, d - 1], x, partner)

    def wait_foth():
        for h in range(chains):
            for d in range(1, n_row):
                took(foth.at[d - 1, 0, h], foth_core.at[h, d - 1])

    def relay_fin():
        for h in range(chains):
            took(fin.at[0, h, pl.ds(0, chips - 1)], fin_sem.at[h])
            put(fin.at[core, h], fin.at[core, h], fin_core_left.at[h], fin_core.at[h], x, partner)

    def send_sums(c):
        for d in range(1, n_row):
            theirs = jnp.concatenate(
                [
                    jnp.concatenate([foth[d - 1, c, h, g * gr + j] for j in range(gr)], axis=1)
                    for h in range(chains) for g in range(gs)
                ],
                axis=0,
            )
            for i, at in enumerate(spans):
                there = slice(at.start - ahead, at.stop - ahead)
                qsend[d - 1, c, :, there] = nn(theirs, a_vm[:, at]).astype(BF)
                put(
                    qsend.at[d - 1, c, :, there], qrecv.at[d - 1, c, :, there], q_left, q_sem.at[d - 1, c, i],
                    row_from(d), col,
                )

    for h in range(chains):
        left_later(foth.at[:, 0, h], foth_core_left.at[h])
        left_later(fin.at[0, h], fin_core_left.at[h])

    @pl.when(core == 1)
    def _():
        relay_foth()

    @pl.when(core == 0)
    def _():
        wait_foth()

    send_sums(1)

    @pl.when(core == 1)
    def _():
        relay_fin()
        wait_foth()

    @pl.when(core == 0)
    def _():
        relay_foth()
        relay_fin()

    send_sums(0)
    left_later(qsend, q_left)

    for h in range(chains):
        took(fin.at[0, h], fin_core.at[h])
    took(cur_recv.at[0], cur_sem)

    own = joined(fin, x, blocks)
    last_hi, last_lo = split(jnp.concatenate([cur_recv[0], cur_recv[1]], axis=0))

    def finish(at, extra):
        marked = onehot[iters - 2, :, at]
        stepped = nn(last_hi, marked) + nn(last_lo, marked)
        stepped = stepped + STEP_SIZE * (nn(own, a_vm[:, at]) + extra)
        out_ref[:, at] = stepped * keep[:, at]
        squares = jnp.sum(stepped * stepped, axis=0, keepdims=True)
        for j in range(at.start // 128, at.stop // 128):
            nrm_send[j] = squares[:, j * 128 - at.start:(j + 1) * 128 - at.start]

    if ahead:
        took(a_peer, ap_sem)
        peers = [joined(fin, row_from(d), blocks) for d in range(1, n_row)]
        for at in cut(0, ahead):
            finish(at, sum(nn(peers[d - 1], a_peer[d - 1, :, at]) for d in range(1, n_row)))
        for d in range(1, n_row):
            piece = pl.ds(0, near)
            put(nrm_send.at[piece], nrm_recv.at[d - 1, piece], nrm_left.at[0], nrm_sem.at[0], row_at(d), col)
        left_later(nrm_recv.at[:, pl.ds(0, near)], nrm_left.at[0])
        left_later(a_peer, ap_left)

    took(e_recv, e_sem.at[0])
    total = e_send[...] + sum(e_recv[k] for k in range(n_row * chips - 1))
    e_both[0] = total
    put(e_both.at[0], e_both.at[1], e_left.at[1], e_sem.at[1], x, partner)
    left_later(e_both.at[0], e_left.at[1])

    for i, at in enumerate(spans):
        there = slice(at.start - ahead, at.stop - ahead)
        for d in range(1, n_row):
            for c in (1, 0):
                took(qrecv.at[d - 1, c, :, there], q_sem.at[d - 1, c, i])
        finish(at, sum(
            jnp.concatenate([qrecv[d - 1, c, :, there] for c in range(2)], axis=0).astype(F32)
            for d in range(1, n_row)
        ))
    for d in range(1, n_row):
        piece = pl.ds(near, lines - near)
        put(nrm_send.at[piece], nrm_recv.at[d - 1, piece], nrm_left.at[1], nrm_sem.at[1], row_at(d), col)
    left_later(nrm_recv.at[:, pl.ds(near, lines - near)], nrm_left.at[1])

    took(e_both.at[1], e_sem.at[1])
    for t in range(iters):
        sums_ref[columns // 128 + t:columns // 128 + t + 1] = e_both[0, t] + e_both[1, t]
    if ahead:
        took(nrm_recv.at[:, pl.ds(0, near)], nrm_sem.at[0])
    took(nrm_recv.at[:, pl.ds(near, lines - near)], nrm_sem.at[1])
    for i in range(lines):
        squares = nrm_send[i] + sum(nrm_recv[d - 1, i] for d in range(1, n_row))
        sums_ref[i:i + 1] = jnp.sqrt(squares)

    for ref, sem in sent:
        took(ref, sem)

    @pl.when(owner_row == x)
    def _():
        for h in range(chains):
            for d in range(1, n_row):
                mp_copy(d, h).wait_send()

    @pl.when(to_row != x)
    def _():
        for h in range(chains):
            first_copy(h).wait_send()

    @pl.when(away > 0)
    def _():
        for h in range(chains):
            took(fin.at[0, h], foth_left.at[h])


def deliver(entries, est_ref, sums_ref, est_out, norm_out, energy_out, sem):
    parts = 4
    rows = est_ref.shape[0] // parts
    lines = norm_out.shape[0]
    copies = [pltpu.make_async_copy(sums_ref.at[pl.ds(0, lines)], norm_out, sem.at[parts])] + [
        pltpu.make_async_copy(
            est_ref.at[pl.ds(i * rows, rows)], est_out.at[pl.ds(i * rows, rows)], sem.at[i]
        )
        for i in range(parts)
    ]
    for copy in copies:
        copy.start()
    for t in range(energy_out.shape[0]):
        energy_out[t] = jnp.sum(sums_ref[lines + t:lines + t + 1]) / entries
    for copy in copies:
        copy.wait()


def local(matrix, measured, support):
    signals, mb = measured.shape
    columns = matrix.shape[1]
    iters = support.shape[0]
    n_row = lax.axis_size("row")
    n_col = lax.axis_size("col")
    s = sizes(n_row, n_col, signals, mb, columns, iters)
    chips, mine, ps, pm, gs, gr, half = (s[k] for k in ("chips", "mine", "ps", "pm", "gs", "gr", "half"))
    chains = s["chains"]
    late = len(cut(s["ahead"], columns))
    rest = columns - s["ahead"]
    lines = columns // 128
    peers = n_row - 1
    dma = pltpu.SemaphoreType.DMA
    vm = pltpu.VMEM
    outs = pl.pallas_call(
        functools.partial(kernel, s),
        out_shape=(
            pltpu.VMEM((half, columns), F32),
            pltpu.VMEM((columns // 128 + (iters + 7) // 8 * 8, 128), F32),
        ),
        in_specs=[
            pl.BlockSpec(memory_space=pltpu.HBM),
            pl.BlockSpec(memory_space=pltpu.HBM),
            pl.BlockSpec(memory_space=pltpu.HBM),
        ],
        out_specs=(pl.BlockSpec(memory_space=vm), pl.BlockSpec(memory_space=vm)),
        scratch_shapes=[
            vm((mb, columns), BF),
            vm(support.shape, support.dtype),
            vm(measured.shape, F32),
            vm((chains, ps, pm), F32),
            vm((iters - 1, KMAX, columns), BF),
            vm((iters - 1, 2 * KMAX, 2 * KMAX), BF),
            vm((iters - 1, n_row, 2 * KMAX, mb), BF),
            vm((2, n_row, mine, KMAX), BF),
            vm((2 * n_row, n_row, mine, KMAX), BF),
            vm((iters - 1, chains, chips, ps, pm), BF),
            vm((iters - 1, chains, chips - 1, ps, pm), BF),
            vm((chains, ps, pm), BF),
            vm((iters - 1, chains, chips, ps, pm), BF),
            vm((2, chains, chips, ps, pm), BF),
            vm((peers, 2, chains, gs * gr, ps, pm), BF),
            vm((2, mine, KMAX), F32),
            vm((2, mine, KMAX), F32),
            vm((peers, 2, mine, rest), BF),
            vm((peers, 2, mine, rest), BF),
            vm((peers, mb, max(s["ahead"], 128)), BF),
            vm((lines, 1, 128), F32),
            vm((peers, lines, 1, 128), F32),
            vm((iters, 1, 128), F32),
            vm((n_row * chips - 1, iters, 1, 128), F32),
            vm((2, iters, 1, 128), F32),
            dma((2,)),
            dma((4,)),
            dma((chains,)),
            dma((peers, chains)),
            dma((iters - 1, 3)),
            dma,
            dma((iters - 1, chains)),
            dma((iters - 1, chains)),
            dma((chains,)),
            dma((chains,)),
            dma((chains,)),
            dma((chains,)),
            dma((chains,)),
            dma,
            dma,
            dma,
            dma((2,)),
            dma((2,)),
            dma((iters - 1, peers)),
            dma((iters - 1, n_row)),
            dma,
            dma((iters - 1, chains)),
            dma((iters - 1, chains)),
            dma((chains,)),
            dma((chains,)),
            dma((chains,)),
            dma((chains, peers)),
            dma,
            dma((peers, 2, late)),
            dma,
            dma((2,)),
            dma((2,)),
        ],
        compiler_params=pltpu.CompilerParams(
            collective_id=0, has_side_effects=True, vmem_limit_bytes=60 * 1024 * 1024
        ),
    )(support, measured, matrix)
    estimate, norms, energy = pl.pallas_call(
        functools.partial(deliver, signals * mb * n_row),
        out_shape=(
            jax.ShapeDtypeStruct((half, columns), F32),
            jax.ShapeDtypeStruct((columns // 128, 128), F32),
            jax.ShapeDtypeStruct((iters,), F32),
        ),
        in_specs=[pl.BlockSpec(memory_space=vm), pl.BlockSpec(memory_space=vm)],
        out_specs=(
            pl.BlockSpec(memory_space=pltpu.HBM), pl.BlockSpec(memory_space=pltpu.HBM),
            pl.BlockSpec(memory_space=pltpu.SMEM),
        ),
        scratch_shapes=[dma((5,))],
        compiler_params=pltpu.CompilerParams(vmem_limit_bytes=8 * 1024 * 1024),
    )(*outs)
    return estimate, norms.reshape(columns), energy


def solution(mesh):
    placed = (P("row", "col"), P(None, "row"), P())
    return jax.shard_map(
        local,
        mesh=mesh,
        in_specs=placed,
        out_specs=(P("row", "col"), P("col"), P()),
        check_vma=False,
    )
```

```python
import functools

import jax
import jax.numpy as jnp
from jax import lax
from jax.experimental import pallas as pl
from jax.experimental.pallas import tpu as pltpu
from jax.sharding import PartitionSpec as P

MESH = pl.DeviceIdType.MESH
KMAX = 128
STEP_SIZE = 0.25
CHUNK = 256
AHEAD = 768
LATE = 0
BF = jnp.bfloat16
F32 = jnp.float32
NT = (((1,), (1,)), ((), ()))


def nn(a, b):
    return jnp.dot(a, b, preferred_element_type=F32)


def nt(a, b):
    return lax.dot_general(a, b, NT, preferred_element_type=F32)


def split(v):
    hi = v.astype(BF)
    return hi, (v - hi.astype(F32)).astype(BF)


def sizes(n_row, n_col, signals, mb, columns, iterations):
    chips = n_col // 2
    mine = signals // n_row // 2
    chains = 2 if mine % 32 == 0 else 1
    sub = mine // chains
    groups = max(1, min(sub // 16, chips))
    parts = chips // groups
    total = mb * n_row
    return dict(
        n_row=n_row, chips=chips, mine=mine, chains=chains, sub=sub, gs=groups, gm=parts,
        ps=sub // groups, pm=total // parts, mb=mb, columns=columns, iters=iterations,
        half=signals // n_row, signals=signals, gr=parts // n_row,
        ahead=min(AHEAD, columns // 2) if n_row == 2 else 0,
    )


def cut(start, stop):
    edges = list(range(start, stop, CHUNK)) + [stop]
    if edges[-1] - edges[-2] > 128:
        edges.insert(-1, edges[-1] - 128)
    return [slice(a, b) for a, b in zip(edges[:-1], edges[1:])]


def kernel(
    s, supp_hbm, meas_hbm, a_ref, out_ref, sums_ref,
    a_vm, supp_ref, meas_ref, mpiece, onehot, same, kept, part_send, part_recv, img, rs, first_out, res, fin, foth,
    cur_send, cur_recv, qsend, qrecv, a_peer, nrm_send, nrm_recv, e_send, e_recv, e_both,
    in_sem, a_sem, mp_sem, mp_left, kept_left, part_left, rs_left, ag_left, first_left, fin_left, fin_core_left,
    foth_left, foth_core_left, cur_left, q_left, ap_left, nrm_left, e_left,
    kept_recv, kept_core, part_sem, rs_sem, ag_sem, fin_sem, fin_core, foth_sem, foth_core,
    cur_sem, q_sem, ap_sem, nrm_sem, e_sem,
):
    n_row, chips, mine, gs, gm, ps, pm = (s[k] for k in ("n_row", "chips", "mine", "gs", "gm", "ps", "pm"))
    chains, sub = s["chains"], s["sub"]
    mb, columns, iters, half, gr, ahead = (s[k] for k in ("mb", "columns", "iters", "half", "gr", "ahead"))
    x = lax.axis_index("row")
    col = lax.axis_index("col")
    chip = col // 2
    core = col % 2
    other = 1 - core
    sent = []

    def put(src, dst, left, recv, row, column):
        pltpu.make_async_remote_copy(
            src_ref=src, dst_ref=dst, send_sem=left, recv_sem=recv,
            device_id={"row": row, "col": column}, device_id_type=MESH,
        ).start()

    def took(ref, sem):
        pltpu.make_async_copy(ref, ref, sem).wait()

    def left_later(ref, sem):
        sent.append((ref, sem))

    def row_at(d):
        return lax.rem(x + d, n_row)

    def row_from(d):
        return lax.rem(x + n_row - d, n_row)

    def chip_at(k):
        return lax.rem(chip + k, chips)

    partner = chip * 2 + other

    supp_load = pltpu.make_async_copy(supp_hbm, supp_ref, in_sem.at[0])
    supp_load.start()
    strips = 4
    strip = mb // strips
    loads = [
        pltpu.make_async_copy(a_ref.at[pl.ds(i * strip, strip)], a_vm.at[pl.ds(i * strip, strip)], a_sem.at[i])
        for i in range(strips)
    ]
    for load in loads:
        load.start()

    meas_load = pltpu.make_async_copy(meas_hbm, meas_ref, in_sem.at[1])
    meas_load.start()

    barrier = pltpu.get_barrier_semaphore()
    greeted = 0
    for d in range(n_row):
        for k in range(chips):
            if d or k:
                pl.semaphore_signal(
                    barrier, inc=1, device_id={"row": row_at(d), "col": chip_at(k) * 2 + core}, device_id_type=MESH
                )
                greeted += 1
        pl.semaphore_signal(barrier, inc=1, device_id={"row": row_at(d), "col": partner}, device_id_type=MESH)
        greeted += 1

    k_all = supp_ref.shape[1]
    lane_k = lax.broadcasted_iota(jnp.int32, (1, k_all), 1).astype(F32)
    slot_k = lax.broadcasted_iota(jnp.int32, (KMAX, k_all), 0).astype(F32)
    eye = lax.broadcasted_iota(jnp.int32, (KMAX, KMAX), 0) == lax.broadcasted_iota(jnp.int32, (KMAX, KMAX), 1)
    lane_n = lax.broadcasted_iota(jnp.int32, (1, columns), 1).astype(F32)

    def window(t, block):
        row = supp_ref[pl.ds(t, 1), :].astype(F32)
        start = (block * columns).astype(F32)
        below = jnp.sum((row < start).astype(F32), axis=1, keepdims=True)
        inside = (row >= start) & (row < start + columns)
        chosen = ((lane_k - below) == slot_k) & inside
        return jnp.sum(jnp.where(chosen, row + 1.0, 0.0), axis=1, keepdims=True) - 1.0

    def as_row(index):
        return jnp.sum(jnp.where(eye, index, 0.0), axis=0, keepdims=True)

    def marks(t):
        return (window(t, col) - (col * columns).astype(F32)) == lane_n

    def place_onehot(t):
        onehot[t] = jnp.where(marks(t), 1.0, 0.0).astype(BF)

    my_slots = pl.ds(pl.multiple_of(core * KMAX, KMAX), KMAX)

    def gather_kept(t):
        if t == 0:
            for load in loads:
                load.wait()
        for i in range(0, mb, 128):
            picked = nt(onehot[t], a_vm[i:i + 128, :])
            kept[t, x, my_slots, i:i + 128] = picked.astype(BF)

    def send_kept(t):
        mine_kept = kept.at[t, x, my_slots]
        put(mine_kept, mine_kept, kept_left.at[t, 0], kept_core.at[t, 0], x, partner)
        left_later(kept.at[t, 0, pl.ds(0, KMAX)], kept_left.at[t, 0])
        if t:
            for d in range(1, n_row):
                put(mine_kept, mine_kept, kept_left.at[t, 1], kept_recv.at[t, d - 1], row_at(d), col)
            pieces = kept.at[t, pl.ds(0, n_row - 1), pl.ds(0, KMAX)]
            left_later(pieces, kept_left.at[t, 1])
            left_later(pieces, kept_left.at[t, 2])

    def relay_kept(t):
        for d in range(1, n_row):
            got = kept.at[t, row_from(d), my_slots]
            took(got, kept_recv.at[t, d - 1])
            put(got, got, kept_left.at[t, 2], kept_core.at[t, d], x, partner)

    def wait_kept(t):
        for d in range(n_row if t else 1):
            took(kept.at[t, 0, pl.ds(0, KMAX)], kept_core.at[t, d])

    supp_load.wait()
    place_onehot(0)
    gather_kept(0)
    pl.semaphore_wait(barrier, greeted)
    send_kept(0)

    meas_load.wait()
    kept_mine = kept[0, x, my_slots, :]
    part = nt(meas_ref[...].astype(BF), kept_mine).astype(BF)
    for r in range(n_row):
        for c in range(2):
            base = r * half + c * mine
            part_send[c, r] = part[base:base + mine]
    for d in range(n_row):
        if d:
            put(part_send.at[core], part_recv.at[2 * d + core], part_left, part_sem, row_at(d), col)
        put(part_send.at[other], part_recv.at[2 * d + core], part_left, part_sem, row_at(d), partner)
    left_later(part_recv.at[pl.ds(0, 2 * n_row - 1)], part_left)
    part_recv[core] = part_send[core]

    def piece_of(j):
        return (j // gm) * gm + lax.rem(lax.rem(j, gm) + core * gr, gm)

    my_piece = piece_of(chip)
    gi = my_piece // gm
    gj = lax.rem(my_piece, gm)
    owner_row = gj // gr
    piece_lane = pl.ds(pl.multiple_of(lax.rem(gj, gr) * pm, 128), pm)

    def piece_rows(r, h):
        return pl.ds(pl.multiple_of(r * half + core * mine + h * sub + gi * ps, 8), ps)

    def mp_copy(d, h):
        return pltpu.make_async_remote_copy(
            src_ref=meas_ref.at[piece_rows(row_at(d), h), piece_lane], dst_ref=mpiece.at[h],
            send_sem=mp_left.at[d - 1, h], recv_sem=mp_sem.at[h],
            device_id={"row": row_at(d), "col": col}, device_id_type=MESH,
        )

    @pl.when(owner_row == x)
    def _():
        for h in range(chains):
            mpiece[h] = meas_ref[piece_rows(x, h), piece_lane]
            for d in range(1, n_row):
                mp_copy(d, h).start()

    place_onehot(1)
    gather_kept(1)
    send_kept(1)

    def global_row(t):
        return jnp.concatenate([as_row(window(t, chip * 2)), as_row(window(t, chip * 2 + 1))], axis=1)

    def global_col(t):
        return jnp.concatenate([window(t, chip * 2), window(t, chip * 2 + 1)], axis=0)

    def same_slots(t):
        row = global_row(t)
        return jnp.where((global_col(t - 1) == row) & (row >= 0.0), 1.0, 0.0).astype(BF)

    def energy(v):
        return jnp.sum(v * v, axis=0, keepdims=True)

    lines = columns // 128
    near = ahead // 128
    early = max(near - LATE, 0)

    def prefetch(i):
        for d in range(1, n_row):
            piece = pl.ds(i * 128, 128)
            put(a_vm.at[:, piece], a_peer.at[d - 1, :, piece], ap_left, ap_sem, row_at(d), col)

    turn = chip // n_row
    to_row = lax.rem(chip + core, n_row)
    first_group = turn // gr
    first_part = lax.rem(turn, gr)
    first_slot = first_group * gm + x * gr + first_part
    first_lane = pl.ds(pl.multiple_of(first_part * pm, 128), pm)

    def first_copy(h):
        return pltpu.make_async_remote_copy(
            src_ref=first_out.at[h], dst_ref=res.at[1, h, first_slot],
            send_sem=first_left.at[h], recv_sem=ag_sem.at[0, h],
            device_id={"row": to_row, "col": col}, device_id_type=MESH,
        )

    def sum_of(t, h):
        took(rs.at[t, h], rs_sem.at[t, h])
        return img[t, h, my_piece if t else chip].astype(F32) + sum(rs[t, h, k].astype(F32) for k in range(chips - 1))

    def scatter(t, h):
        for k in range(1, chips):
            put(
                img.at[t, h, piece_of(chip_at(k)) if t else chip_at(k)], rs.at[t, h, k - 1], rs_left.at[t, h], rs_sem.at[t, h],
                x, chip_at(k) * 2 + core,
            )
        left_later(rs.at[t, h], rs_left.at[t, h])

    def joined(buffer, r, blocks):
        return jnp.concatenate(
            [
                jnp.concatenate([buffer[b + (g * gm + r * gr + j,)] for j in range(gr)], axis=1)
                for b in blocks for g in range(gs)
            ],
            axis=0,
        )

    took(part_recv.at[pl.ds(0, 2 * n_row - 1)], part_sem)

    def first_step(rows):
        return STEP_SIZE * jnp.concatenate(
            [sum(part_recv[(2 * d + b,) + rows].astype(F32) for d in range(n_row)) for b in range(2)], axis=-1
        )

    wait_kept(0)
    for h in range(chains):
        at = slice(h * sub, (h + 1) * sub)
        rounded = jnp.concatenate([first_step((r, at)) for r in range(n_row)], axis=0).astype(BF)
        image = nn(rounded, kept[0, x]).astype(BF)
        for r in range(n_row):
            for g in range(gs):
                for j in range(gr):
                    place = (g * gr + j) * n_row + lax.rem(r + n_row - lax.rem(core, n_row), n_row)
                    img[0, h, place] = image[
                        r * sub + g * ps:r * sub + (g + 1) * ps, j * pm:(j + 1) * pm
                    ]
        scatter(0, h)
    for t in range(2, iters - 1):
        place_onehot(t)
        gather_kept(t)
        send_kept(t)
    mine_step = first_step((x,))
    current = [mine_step[h * sub:(h + 1) * sub] for h in range(chains)]

    @pl.when(owner_row != x)
    def _():
        for h in range(chains):
            took(mpiece.at[h], mp_sem.at[h])

    energies = [[energy(mpiece[h]) for h in range(chains)]]
    for u in range(1, iters - 1):
        same[u] = same_slots(u)
    keep = jnp.sum(jnp.where(marks(iters - 1), 1.0, 0.0), axis=0, keepdims=True)

    found = []
    for h in range(chains):
        rows = pl.ds(pl.multiple_of(to_row * half + core * mine + h * sub + first_group * ps, 8), ps)
        residual = meas_ref[rows, first_lane] - sum_of(0, h)
        found.append(energy(residual))
        first_out[h] = residual.astype(BF)
        for k in range(1, chips):
            put(
                first_out.at[h], res.at[1, h, first_slot], ag_left.at[0, h], ag_sem.at[0, h],
                to_row, chip_at(k) * 2 + core,
            )
        left_later(rs.at[0, 0], ag_left.at[0, h])

        @pl.when(to_row == x)
        def _():
            res[1, h, first_slot] = first_out[h]

        @pl.when(to_row != x)
        def _():
            first_copy(h).start()

    energies.append(found)
    relay_kept(1)
    for i in range(early):
        prefetch(i)
    wait_kept(1)

    away = lax.rem(owner_row + n_row - x, n_row)
    slot = gi * gr + lax.rem(gj, gr)

    def foth_copy(h, k):
        return pltpu.make_async_remote_copy(
            src_ref=fin.at[core, h, my_piece], dst_ref=foth.at[jnp.maximum(away - 1, 0), core, h, slot],
            send_sem=foth_left.at[h], recv_sem=foth_sem.at[h],
            device_id={"row": owner_row, "col": chip_at(k) * 2 + core}, device_id_type=MESH,
        )

    for t in range(1, iters - 1):
        carried = []
        for h in range(chains):
            hi, lo = split(current[h])
            carried.append(nn(hi, same[t]) + nn(lo, same[t]))
        for h in range(chains):
            if t == 1:

                @pl.when(to_row == x)
                def _():
                    took(res.at[1, h, pl.ds(0, chips - 1)], ag_sem.at[0, h])

                @pl.when(to_row != x)
                def _():
                    took(res.at[1, h], ag_sem.at[0, h])

            else:
                took(res.at[1, h, pl.ds(0, chips - 1)], ag_sem.at[t - 1, h])
            gradient = sum(nt(joined(res, r, [(t, h)]), kept[t, r]) for r in range(n_row))
            current[h] = carried[h] + STEP_SIZE * gradient
            rounded = current[h].astype(BF)
            for r in range(n_row):
                image = nn(rounded, kept[t, r]).astype(BF)
                for g in range(gs):
                    for j in range(gr):
                        img[t, h, g * gm + r * gr + j] = image[g * ps:(g + 1) * ps, j * pm:(j + 1) * pm]
            scatter(t, h)
        if t + 1 < iters - 1:
            relay_kept(t + 1)
            wait_kept(t + 1)
        found = []
        for h in range(chains):
            residual = mpiece[h] - sum_of(t, h)
            found.append(energy(residual))
            if t < iters - 2:
                res[t + 1, h, my_piece] = residual.astype(BF)
                piece = res.at[t + 1, h, my_piece]
                for k in range(1, chips):
                    put(piece, piece, ag_left.at[t, h], ag_sem.at[t, h], x, chip_at(k) * 2 + core)
                left_later(rs.at[0, 0], ag_left.at[t, h])
                continue
            fin[core, h, my_piece] = residual.astype(BF)

            @pl.when(away > 0)
            def _():
                for k in range(chips):
                    foth_copy(h, k).start()

            if h == chains - 1:
                for i in range(early, near):
                    prefetch(i)
            piece = fin.at[core, h, my_piece]
            for k in range(1, chips):
                put(piece, piece, fin_left.at[h], fin_sem.at[h], x, chip_at(k) * 2 + core)
            left_later(rs.at[0, 0], fin_left.at[h])
        energies.append(found)

    lanes = e_send.shape[2]
    folded = [
        sum(e[:, i * lanes:(i + 1) * lanes] for e in found for i in range(pm // lanes)) for found in energies
    ]
    for t in range(iters):
        e_send[t] = folded[t]
    for d in range(n_row):
        for k in range(chips):
            if d or k:
                put(e_send, e_recv.at[d * chips + k - 1], e_left.at[0], e_sem.at[0], row_at(d), chip_at(k) * 2 + core)

    left_later(e_recv, e_left.at[0])

    for b in range(2):
        for h in range(chains):
            cur_send[b, h * sub:(h + 1) * sub] = current[h][:, b * KMAX:(b + 1) * KMAX]
    put(cur_send.at[other], cur_recv.at[core], cur_left, cur_sem, x, partner)
    left_later(cur_recv.at[0], cur_left)
    cur_recv[core] = cur_send[core]

    spans = cut(ahead, columns)
    blocks = [(c, h) for c in range(2) for h in range(chains)]

    def relay_foth():
        for h in range(chains):
            took(foth.at[:, 0, h], foth_sem.at[h])
            for d in range(1, n_row):
                got = foth.at[d - 1, core, h]
                put(got, got, foth_core_left.at[h], foth_core.at[h, d - 1], x, partner)

    def wait_foth():
        for h in range(chains):
            for d in range(1, n_row):
                took(foth.at[d - 1, 0, h], foth_core.at[h, d - 1])

    def relay_fin():
        for h in range(chains):
            took(fin.at[0, h, pl.ds(0, chips - 1)], fin_sem.at[h])
            put(fin.at[core, h], fin.at[core, h], fin_core_left.at[h], fin_core.at[h], x, partner)

    def send_sums(c):
        for d in range(1, n_row):
            theirs = jnp.concatenate(
                [
                    jnp.concatenate([foth[d - 1, c, h, g * gr + j] for j in range(gr)], axis=1)
                    for h in range(chains) for g in range(gs)
                ],
                axis=0,
            )
            for i, at in enumerate(spans):
                there = slice(at.start - ahead, at.stop - ahead)
                qsend[d - 1, c, :, there] = nn(theirs, a_vm[:, at]).astype(BF)
                put(
                    qsend.at[d - 1, c, :, there], qrecv.at[d - 1, c, :, there], q_left, q_sem.at[d - 1, i],
                    row_from(d), col,
                )

    for h in range(chains):
        left_later(foth.at[:, 0, h], foth_core_left.at[h])
        left_later(fin.at[0, h], fin_core_left.at[h])

    @pl.when(core == 1)
    def _():
        relay_foth()

    @pl.when(core == 0)
    def _():
        wait_foth()

    send_sums(1)

    @pl.when(core == 1)
    def _():
        relay_fin()
        wait_foth()

    @pl.when(core == 0)
    def _():
        relay_foth()
        relay_fin()

    send_sums(0)
    left_later(qsend, q_left)

    for h in range(chains):
        took(fin.at[0, h], fin_core.at[h])
    took(cur_recv.at[0], cur_sem)

    own = joined(fin, x, blocks)
    last_hi, last_lo = split(jnp.concatenate([cur_recv[0], cur_recv[1]], axis=0))

    def finish(at, extra):
        marked = onehot[iters - 2, :, at]
        stepped = nn(last_hi, marked) + nn(last_lo, marked)
        stepped = stepped + STEP_SIZE * (nn(own, a_vm[:, at]) + extra)
        out_ref[:, at] = stepped * keep[:, at]
        squares = jnp.sum(stepped * stepped, axis=0, keepdims=True)
        for j in range(at.start // 128, at.stop // 128):
            nrm_send[j] = squares[:, j * 128 - at.start:(j + 1) * 128 - at.start]

    if ahead:
        took(a_peer, ap_sem)
        peers = [joined(fin, row_from(d), blocks) for d in range(1, n_row)]
        for at in cut(0, ahead):
            finish(at, sum(nn(peers[d - 1], a_peer[d - 1, :, at]) for d in range(1, n_row)))
        for d in range(1, n_row):
            piece = pl.ds(0, near)
            put(nrm_send.at[piece], nrm_recv.at[d - 1, piece], nrm_left.at[0], nrm_sem.at[0], row_at(d), col)
        left_later(nrm_recv.at[:, pl.ds(0, near)], nrm_left.at[0])
        left_later(a_peer, ap_left)

    took(e_recv, e_sem.at[0])
    total = e_send[...] + sum(e_recv[k] for k in range(n_row * chips - 1))
    e_both[0] = total
    put(e_both.at[0], e_both.at[1], e_left.at[1], e_sem.at[1], x, partner)
    left_later(e_both.at[0], e_left.at[1])

    for i, at in enumerate(spans):
        there = slice(at.start - ahead, at.stop - ahead)
        for d in range(1, n_row):
            took(qrecv.at[d - 1, :, :, there], q_sem.at[d - 1, i])
        finish(at, sum(
            jnp.concatenate([qrecv[d - 1, c, :, there] for c in range(2)], axis=0).astype(F32)
            for d in range(1, n_row)
        ))
    for d in range(1, n_row):
        piece = pl.ds(near, lines - near)
        put(nrm_send.at[piece], nrm_recv.at[d - 1, piece], nrm_left.at[1], nrm_sem.at[1], row_at(d), col)
    left_later(nrm_recv.at[:, pl.ds(near, lines - near)], nrm_left.at[1])

    took(e_both.at[1], e_sem.at[1])
    for t in range(iters):
        sums_ref[columns // 128 + t:columns // 128 + t + 1] = e_both[0, t] + e_both[1, t]
    if ahead:
        took(nrm_recv.at[:, pl.ds(0, near)], nrm_sem.at[0])
    took(nrm_recv.at[:, pl.ds(near, lines - near)], nrm_sem.at[1])
    for i in range(lines):
        squares = nrm_send[i] + sum(nrm_recv[d - 1, i] for d in range(1, n_row))
        sums_ref[i:i + 1] = jnp.sqrt(squares)

    for ref, sem in sent:
        took(ref, sem)

    @pl.when(owner_row == x)
    def _():
        for h in range(chains):
            for d in range(1, n_row):
                mp_copy(d, h).wait_send()

    @pl.when(to_row != x)
    def _():
        for h in range(chains):
            first_copy(h).wait_send()

    @pl.when(away > 0)
    def _():
        for h in range(chains):
            took(fin.at[0, h], foth_left.at[h])


def deliver(entries, est_ref, sums_ref, est_out, norm_out, energy_out, sem):
    parts = 8
    rows = est_ref.shape[0] // parts
    lines = norm_out.shape[0]
    copies = [pltpu.make_async_copy(sums_ref.at[pl.ds(0, lines)], norm_out, sem.at[parts])] + [
        pltpu.make_async_copy(
            est_ref.at[pl.ds(i * rows, rows)], est_out.at[pl.ds(i * rows, rows)], sem.at[i]
        )
        for i in range(parts)
    ]
    for copy in copies:
        copy.start()
    for t in range(energy_out.shape[0]):
        energy_out[t] = jnp.sum(sums_ref[lines + t:lines + t + 1]) / entries
    for copy in copies:
        copy.wait()


def local(matrix, measured, support):
    signals, mb = measured.shape
    columns = matrix.shape[1]
    iters = support.shape[0]
    n_row = lax.axis_size("row")
    n_col = lax.axis_size("col")
    s = sizes(n_row, n_col, signals, mb, columns, iters)
    chips, mine, ps, pm, gs, gr, half = (s[k] for k in ("chips", "mine", "ps", "pm", "gs", "gr", "half"))
    chains = s["chains"]
    late = len(cut(s["ahead"], columns))
    rest = columns - s["ahead"]
    lines = columns // 128
    peers = n_row - 1
    dma = pltpu.SemaphoreType.DMA
    vm = pltpu.VMEM
    outs = pl.pallas_call(
        functools.partial(kernel, s),
        out_shape=(
            pltpu.VMEM((half, columns), F32),
            pltpu.VMEM((columns // 128 + (iters + 7) // 8 * 8, 128), F32),
        ),
        in_specs=[
            pl.BlockSpec(memory_space=pltpu.HBM),
            pl.BlockSpec(memory_space=pltpu.HBM),
            pl.BlockSpec(memory_space=pltpu.HBM),
        ],
        out_specs=(pl.BlockSpec(memory_space=vm), pl.BlockSpec(memory_space=vm)),
        scratch_shapes=[
            vm((mb, columns), BF),
            vm(support.shape, support.dtype),
            vm(measured.shape, F32),
            vm((chains, ps, pm), F32),
            vm((iters - 1, KMAX, columns), BF),
            vm((iters - 1, 2 * KMAX, 2 * KMAX), BF),
            vm((iters - 1, n_row, 2 * KMAX, mb), BF),
            vm((2, n_row, mine, KMAX), BF),
            vm((2 * n_row, n_row, mine, KMAX), BF),
            vm((iters - 1, chains, chips, ps, pm), BF),
            vm((iters - 1, chains, chips - 1, ps, pm), BF),
            vm((chains, ps, pm), BF),
            vm((iters - 1, chains, chips, ps, pm), BF),
            vm((2, chains, chips, ps, pm), BF),
            vm((peers, 2, chains, gs * gr, ps, pm), BF),
            vm((2, mine, KMAX), F32),
            vm((2, mine, KMAX), F32),
            vm((peers, 2, mine, rest), BF),
            vm((peers, 2, mine, rest), BF),
            vm((peers, mb, max(s["ahead"], 128)), BF),
            vm((lines, 1, 128), F32),
            vm((peers, lines, 1, 128), F32),
            vm((iters, 1, 128), F32),
            vm((n_row * chips - 1, iters, 1, 128), F32),
            vm((2, iters, 1, 128), F32),
            dma((2,)),
            dma((4,)),
            dma((chains,)),
            dma((peers, chains)),
            dma((iters - 1, 3)),
            dma,
            dma((iters - 1, chains)),
            dma((iters - 1, chains)),
            dma((chains,)),
            dma((chains,)),
            dma((chains,)),
            dma((chains,)),
            dma((chains,)),
            dma,
            dma,
            dma,
            dma((2,)),
            dma((2,)),
            dma((iters - 1, peers)),
            dma((iters - 1, n_row)),
            dma,
            dma((iters - 1, chains)),
            dma((iters - 1, chains)),
            dma((chains,)),
            dma((chains,)),
            dma((chains,)),
            dma((chains, peers)),
            dma,
            dma((peers, late)),
            dma,
            dma((2,)),
            dma((2,)),
        ],
        compiler_params=pltpu.CompilerParams(
            collective_id=0, has_side_effects=True, vmem_limit_bytes=60 * 1024 * 1024
        ),
    )(support, measured, matrix)
    estimate, norms, energy = pl.pallas_call(
        functools.partial(deliver, signals * mb * n_row),
        out_shape=(
            jax.ShapeDtypeStruct((half, columns), F32),
            jax.ShapeDtypeStruct((columns // 128, 128), F32),
            jax.ShapeDtypeStruct((iters,), F32),
        ),
        in_specs=[pl.BlockSpec(memory_space=vm), pl.BlockSpec(memory_space=vm)],
        out_specs=(
            pl.BlockSpec(memory_space=pltpu.HBM), pl.BlockSpec(memory_space=pltpu.HBM),
            pl.BlockSpec(memory_space=pltpu.SMEM),
        ),
        scratch_shapes=[dma((9,))],
        compiler_params=pltpu.CompilerParams(vmem_limit_bytes=8 * 1024 * 1024),
    )(*outs)
    return estimate, norms.reshape(columns), energy


def solution(mesh):
    placed = (P("row", "col"), P(None, "row"), P())
    return jax.shard_map(
        local,
        mesh=mesh,
        in_specs=placed,
        out_specs=(P("row", "col"), P("col"), P()),
        check_vma=False,
    )
```

```python
import functools

import jax
import jax.numpy as jnp
from jax import lax
from jax.experimental import pallas as pl
from jax.experimental.pallas import tpu as pltpu
from jax.sharding import PartitionSpec as P

MESH = pl.DeviceIdType.MESH
KMAX = 128
STEP_SIZE = 0.25
CHUNK = 512
AHEAD = 768
LATE = 2
BF = jnp.bfloat16
F32 = jnp.float32
NT = (((1,), (1,)), ((), ()))


def nn(a, b):
    return jnp.dot(a, b, preferred_element_type=F32)


def nt(a, b):
    return lax.dot_general(a, b, NT, preferred_element_type=F32)


def split(v):
    hi = v.astype(BF)
    return hi, (v - hi.astype(F32)).astype(BF)


def sizes(n_row, n_col, signals, mb, columns, iterations):
    chips = n_col // 2
    mine = signals // n_row // 2
    chains = 2 if mine % 32 == 0 else 1
    sub = mine // chains
    groups = max(1, min(sub // 16, chips))
    parts = chips // groups
    total = mb * n_row
    return dict(
        n_row=n_row, chips=chips, mine=mine, chains=chains, sub=sub, gs=groups, gm=parts,
        ps=sub // groups, pm=total // parts, mb=mb, columns=columns, iters=iterations,
        half=signals // n_row, signals=signals, gr=parts // n_row,
        ahead=min(AHEAD, columns // 2) if n_row == 2 else 0,
    )


def cut(start, stop):
    edges = list(range(start, stop, CHUNK)) + [stop]
    if edges[-1] - edges[-2] > 128:
        edges.insert(-1, edges[-1] - 128)
    return [slice(a, b) for a, b in zip(edges[:-1], edges[1:])]


def kernel(
    s, supp_hbm, meas_hbm, a_ref, out_ref, sums_ref,
    a_vm, supp_ref, meas_ref, mpiece, onehot, same, kept, part_send, part_recv, img, rs, first_out, res, fin, foth,
    cur_send, cur_recv, qsend, qrecv, a_peer, nrm_send, nrm_recv, e_send, e_recv, e_both,
    in_sem, a_sem, mp_sem, mp_left, kept_left, part_left, rs_left, ag_left, first_left, fin_left, fin_core_left,
    foth_left, foth_core_left, cur_left, q_left, ap_left, nrm_left, e_left,
    kept_recv, kept_core, part_sem, rs_sem, ag_sem, fin_sem, fin_core, foth_sem, foth_core,
    cur_sem, q_sem, ap_sem, nrm_sem, e_sem,
):
    n_row, chips, mine, gs, gm, ps, pm = (s[k] for k in ("n_row", "chips", "mine", "gs", "gm", "ps", "pm"))
    chains, sub = s["chains"], s["sub"]
    mb, columns, iters, half, gr, ahead = (s[k] for k in ("mb", "columns", "iters", "half", "gr", "ahead"))
    x = lax.axis_index("row")
    col = lax.axis_index("col")
    chip = col // 2
    core = col % 2
    other = 1 - core
    sent = []

    def put(src, dst, left, recv, row, column):
        pltpu.make_async_remote_copy(
            src_ref=src, dst_ref=dst, send_sem=left, recv_sem=recv,
            device_id={"row": row, "col": column}, device_id_type=MESH,
        ).start()

    def took(ref, sem):
        pltpu.make_async_copy(ref, ref, sem).wait()

    def left_later(ref, sem):
        sent.append((ref, sem))

    def row_at(d):
        return lax.rem(x + d, n_row)

    def row_from(d):
        return lax.rem(x + n_row - d, n_row)

    def chip_at(k):
        return lax.rem(chip + k, chips)

    partner = chip * 2 + other

    supp_load = pltpu.make_async_copy(supp_hbm, supp_ref, in_sem.at[0])
    supp_load.start()
    strips = 4
    strip = mb // strips
    loads = [
        pltpu.make_async_copy(a_ref.at[pl.ds(i * strip, strip)], a_vm.at[pl.ds(i * strip, strip)], a_sem.at[i])
        for i in range(strips)
    ]
    for load in loads:
        load.start()

    meas_load = pltpu.make_async_copy(meas_hbm, meas_ref, in_sem.at[1])
    meas_load.start()

    barrier = pltpu.get_barrier_semaphore()
    greeted = 0
    for d in range(n_row):
        for k in range(chips):
            if d or k:
                pl.semaphore_signal(
                    barrier, inc=1, device_id={"row": row_at(d), "col": chip_at(k) * 2 + core}, device_id_type=MESH
                )
                greeted += 1
        pl.semaphore_signal(barrier, inc=1, device_id={"row": row_at(d), "col": partner}, device_id_type=MESH)
        greeted += 1

    k_all = supp_ref.shape[1]
    lane_k = lax.broadcasted_iota(jnp.int32, (1, k_all), 1).astype(F32)
    slot_k = lax.broadcasted_iota(jnp.int32, (KMAX, k_all), 0).astype(F32)
    eye = lax.broadcasted_iota(jnp.int32, (KMAX, KMAX), 0) == lax.broadcasted_iota(jnp.int32, (KMAX, KMAX), 1)
    lane_n = lax.broadcasted_iota(jnp.int32, (1, columns), 1).astype(F32)

    def window(t, block):
        row = supp_ref[pl.ds(t, 1), :].astype(F32)
        start = (block * columns).astype(F32)
        below = jnp.sum((row < start).astype(F32), axis=1, keepdims=True)
        inside = (row >= start) & (row < start + columns)
        chosen = ((lane_k - below) == slot_k) & inside
        return jnp.sum(jnp.where(chosen, row + 1.0, 0.0), axis=1, keepdims=True) - 1.0

    def as_row(index):
        return jnp.sum(jnp.where(eye, index, 0.0), axis=0, keepdims=True)

    def marks(t):
        return (window(t, col) - (col * columns).astype(F32)) == lane_n

    def place_onehot(t):
        onehot[t] = jnp.where(marks(t), 1.0, 0.0).astype(BF)

    my_slots = pl.ds(pl.multiple_of(core * KMAX, KMAX), KMAX)

    def gather_kept(t):
        if t == 0:
            for load in loads:
                load.wait()
        for i in range(0, mb, 128):
            picked = nt(onehot[t], a_vm[i:i + 128, :])
            kept[t, x, my_slots, i:i + 128] = picked.astype(BF)

    def send_kept(t):
        mine_kept = kept.at[t, x, my_slots]
        put(mine_kept, mine_kept, kept_left.at[t, 0], kept_core.at[t, 0], x, partner)
        left_later(kept.at[t, 0, pl.ds(0, KMAX)], kept_left.at[t, 0])
        if t:
            for d in range(1, n_row):
                put(mine_kept, mine_kept, kept_left.at[t, 1], kept_recv.at[t, d - 1], row_at(d), col)
            pieces = kept.at[t, pl.ds(0, n_row - 1), pl.ds(0, KMAX)]
            left_later(pieces, kept_left.at[t, 1])
            left_later(pieces, kept_left.at[t, 2])

    def relay_kept(t):
        for d in range(1, n_row):
            got = kept.at[t, row_from(d), my_slots]
            took(got, kept_recv.at[t, d - 1])
            put(got, got, kept_left.at[t, 2], kept_core.at[t, d], x, partner)

    def wait_kept(t):
        for d in range(n_row if t else 1):
            took(kept.at[t, 0, pl.ds(0, KMAX)], kept_core.at[t, d])

    supp_load.wait()
    place_onehot(0)
    gather_kept(0)
    pl.semaphore_wait(barrier, greeted)
    send_kept(0)

    meas_load.wait()
    kept_mine = kept[0, x, my_slots, :]
    part = nt(meas_ref[...].astype(BF), kept_mine).astype(BF)
    for r in range(n_row):
        for c in range(2):
            base = r * half + c * mine
            part_send[c, r] = part[base:base + mine]
    for d in range(n_row):
        if d:
            put(part_send.at[core], part_recv.at[2 * d + core], part_left, part_sem, row_at(d), col)
        put(part_send.at[other], part_recv.at[2 * d + core], part_left, part_sem, row_at(d), partner)
    left_later(part_recv.at[pl.ds(0, 2 * n_row - 1)], part_left)
    part_recv[core] = part_send[core]

    def piece_of(j):
        return (j // gm) * gm + lax.rem(lax.rem(j, gm) + core * gr, gm)

    my_piece = piece_of(chip)
    gi = my_piece // gm
    gj = lax.rem(my_piece, gm)
    owner_row = gj // gr
    piece_lane = pl.ds(pl.multiple_of(lax.rem(gj, gr) * pm, 128), pm)

    def piece_rows(r, h):
        return pl.ds(pl.multiple_of(r * half + core * mine + h * sub + gi * ps, 8), ps)

    def mp_copy(d, h):
        return pltpu.make_async_remote_copy(
            src_ref=meas_ref.at[piece_rows(row_at(d), h), piece_lane], dst_ref=mpiece.at[h],
            send_sem=mp_left.at[d - 1, h], recv_sem=mp_sem.at[h],
            device_id={"row": row_at(d), "col": col}, device_id_type=MESH,
        )

    @pl.when(owner_row == x)
    def _():
        for h in range(chains):
            mpiece[h] = meas_ref[piece_rows(x, h), piece_lane]
            for d in range(1, n_row):
                mp_copy(d, h).start()

    place_onehot(1)
    gather_kept(1)
    send_kept(1)

    def global_row(t):
        return jnp.concatenate([as_row(window(t, chip * 2)), as_row(window(t, chip * 2 + 1))], axis=1)

    def global_col(t):
        return jnp.concatenate([window(t, chip * 2), window(t, chip * 2 + 1)], axis=0)

    def same_slots(t):
        row = global_row(t)
        return jnp.where((global_col(t - 1) == row) & (row >= 0.0), 1.0, 0.0).astype(BF)

    def energy(v):
        return jnp.sum(v * v, axis=0, keepdims=True)

    lines = columns // 128
    near = ahead // 128
    early = max(near - LATE, 0)

    def prefetch(i):
        for d in range(1, n_row):
            piece = pl.ds(i * 128, 128)
            put(a_vm.at[:, piece], a_peer.at[d - 1, :, piece], ap_left, ap_sem, row_at(d), col)

    turn = chip // n_row
    to_row = lax.rem(chip + core, n_row)
    first_group = turn // gr
    first_part = lax.rem(turn, gr)
    first_slot = first_group * gm + x * gr + first_part
    first_lane = pl.ds(pl.multiple_of(first_part * pm, 128), pm)

    def first_copy(h):
        return pltpu.make_async_remote_copy(
            src_ref=first_out.at[h], dst_ref=res.at[1, h, first_slot],
            send_sem=first_left.at[h], recv_sem=ag_sem.at[0, h],
            device_id={"row": to_row, "col": col}, device_id_type=MESH,
        )

    def sum_of(t, h):
        took(rs.at[t, h], rs_sem.at[t, h])
        return img[t, h, my_piece if t else chip].astype(F32) + sum(rs[t, h, k].astype(F32) for k in range(chips - 1))

    def scatter(t, h):
        for k in range(1, chips):
            put(
                img.at[t, h, piece_of(chip_at(k)) if t else chip_at(k)], rs.at[t, h, k - 1], rs_left.at[t, h], rs_sem.at[t, h],
                x, chip_at(k) * 2 + core,
            )
        left_later(rs.at[t, h], rs_left.at[t, h])

    def joined(buffer, r, blocks):
        return jnp.concatenate(
            [
                jnp.concatenate([buffer[b + (g * gm + r * gr + j,)] for j in range(gr)], axis=1)
                for b in blocks for g in range(gs)
            ],
            axis=0,
        )

    took(part_recv.at[pl.ds(0, 2 * n_row - 1)], part_sem)

    def first_step(rows):
        return STEP_SIZE * jnp.concatenate(
            [sum(part_recv[(2 * d + b,) + rows].astype(F32) for d in range(n_row)) for b in range(2)], axis=-1
        )

    wait_kept(0)
    for h in range(chains):
        at = slice(h * sub, (h + 1) * sub)
        rounded = jnp.concatenate([first_step((r, at)) for r in range(n_row)], axis=0).astype(BF)
        image = nn(rounded, kept[0, x]).astype(BF)
        for r in range(n_row):
            for g in range(gs):
                for j in range(gr):
                    place = (g * gr + j) * n_row + lax.rem(r + n_row - lax.rem(core, n_row), n_row)
                    img[0, h, place] = image[
                        r * sub + g * ps:r * sub + (g + 1) * ps, j * pm:(j + 1) * pm
                    ]
        scatter(0, h)
    for t in range(2, iters - 1):
        place_onehot(t)
        gather_kept(t)
        send_kept(t)
    mine_step = first_step((x,))
    current = [mine_step[h * sub:(h + 1) * sub] for h in range(chains)]

    @pl.when(owner_row != x)
    def _():
        for h in range(chains):
            took(mpiece.at[h], mp_sem.at[h])

    energies = [[energy(mpiece[h]) for h in range(chains)]]
    for u in range(1, iters - 1):
        same[u] = same_slots(u)
    keep = jnp.sum(jnp.where(marks(iters - 1), 1.0, 0.0), axis=0, keepdims=True)

    found = []
    for h in range(chains):
        rows = pl.ds(pl.multiple_of(to_row * half + core * mine + h * sub + first_group * ps, 8), ps)
        residual = meas_ref[rows, first_lane] - sum_of(0, h)
        found.append(energy(residual))
        first_out[h] = residual.astype(BF)
        for k in range(1, chips):
            put(
                first_out.at[h], res.at[1, h, first_slot], ag_left.at[0, h], ag_sem.at[0, h],
                to_row, chip_at(k) * 2 + core,
            )
        left_later(rs.at[0, 0], ag_left.at[0, h])

        @pl.when(to_row == x)
        def _():
            res[1, h, first_slot] = first_out[h]

        @pl.when(to_row != x)
        def _():
            first_copy(h).start()

    energies.append(found)
    relay_kept(1)
    for i in range(early):
        prefetch(i)

    @pl.when(core == 0)
    def _():
        for i in range(early, near):
            prefetch(i)

    wait_kept(1)

    away = lax.rem(owner_row + n_row - x, n_row)
    slot = gi * gr + lax.rem(gj, gr)

    def foth_copy(h, k):
        return pltpu.make_async_remote_copy(
            src_ref=fin.at[core, h, my_piece], dst_ref=foth.at[jnp.maximum(away - 1, 0), core, h, slot],
            send_sem=foth_left.at[h], recv_sem=foth_sem.at[h],
            device_id={"row": owner_row, "col": chip_at(k) * 2 + core}, device_id_type=MESH,
        )

    for t in range(1, iters - 1):
        carried = []
        for h in range(chains):
            hi, lo = split(current[h])
            carried.append(nn(hi, same[t]) + nn(lo, same[t]))
        for h in range(chains):
            if t == 1:

                @pl.when(to_row == x)
                def _():
                    took(res.at[1, h, pl.ds(0, chips - 1)], ag_sem.at[0, h])

                @pl.when(to_row != x)
                def _():
                    took(res.at[1, h], ag_sem.at[0, h])

            else:
                took(res.at[1, h, pl.ds(0, chips - 1)], ag_sem.at[t - 1, h])
            gradient = sum(nt(joined(res, r, [(t, h)]), kept[t, r]) for r in range(n_row))
            current[h] = carried[h] + STEP_SIZE * gradient
            rounded = current[h].astype(BF)
            for r in range(n_row):
                image = nn(rounded, kept[t, r]).astype(BF)
                for g in range(gs):
                    for j in range(gr):
                        img[t, h, g * gm + r * gr + j] = image[g * ps:(g + 1) * ps, j * pm:(j + 1) * pm]
            scatter(t, h)
        if t + 1 < iters - 1:
            relay_kept(t + 1)
            wait_kept(t + 1)
        found = []
        for h in range(chains):
            residual = mpiece[h] - sum_of(t, h)
            found.append(energy(residual))
            if t < iters - 2:
                res[t + 1, h, my_piece] = residual.astype(BF)
                piece = res.at[t + 1, h, my_piece]
                for k in range(1, chips):
                    put(piece, piece, ag_left.at[t, h], ag_sem.at[t, h], x, chip_at(k) * 2 + core)
                left_later(rs.at[0, 0], ag_left.at[t, h])
                continue
            fin[core, h, my_piece] = residual.astype(BF)

            @pl.when(away > 0)
            def _():
                for k in range(chips):
                    foth_copy(h, k).start()

            if h == chains - 1:

                @pl.when(core == 1)
                def _():
                    for i in range(early, near):
                        prefetch(i)

            piece = fin.at[core, h, my_piece]
            for k in range(1, chips):
                put(piece, piece, fin_left.at[h], fin_sem.at[h], x, chip_at(k) * 2 + core)
            left_later(rs.at[0, 0], fin_left.at[h])
        energies.append(found)

    lanes = e_send.shape[2]
    folded = [
        sum(e[:, i * lanes:(i + 1) * lanes] for e in found for i in range(pm // lanes)) for found in energies
    ]
    for t in range(iters):
        e_send[t] = folded[t]
    for d in range(n_row):
        for k in range(chips):
            if d or k:
                put(e_send, e_recv.at[d * chips + k - 1], e_left.at[0], e_sem.at[0], row_at(d), chip_at(k) * 2 + core)

    left_later(e_recv, e_left.at[0])

    for b in range(2):
        for h in range(chains):
            cur_send[b, h * sub:(h + 1) * sub] = current[h][:, b * KMAX:(b + 1) * KMAX]
    put(cur_send.at[other], cur_recv.at[core], cur_left, cur_sem, x, partner)
    left_later(cur_recv.at[0], cur_left)
    cur_recv[core] = cur_send[core]

    spans = cut(ahead, columns)
    blocks = [(c, h) for c in range(2) for h in range(chains)]

    def relay_foth():
        for h in range(chains):
            took(foth.at[:, 0, h], foth_sem.at[h])
            for d in range(1, n_row):
                got = foth.at[d - 1, core, h]
                put(got, got, foth_core_left.at[h], foth_core.at[h, d - 1], x, partner)

    def wait_foth():
        for h in range(chains):
            for d in range(1, n_row):
                took(foth.at[d - 1, 0, h], foth_core.at[h, d - 1])

    def relay_fin():
        for h in range(chains):
            took(fin.at[0, h, pl.ds(0, chips - 1)], fin_sem.at[h])
            put(fin.at[core, h], fin.at[core, h], fin_core_left.at[h], fin_core.at[h], x, partner)

    def send_sums(c):
        for d in range(1, n_row):
            theirs = jnp.concatenate(
                [
                    jnp.concatenate([foth[d - 1, c, h, g * gr + j] for j in range(gr)], axis=1)
                    for h in range(chains) for g in range(gs)
                ],
                axis=0,
            )
            for i, at in enumerate(spans):
                there = slice(at.start - ahead, at.stop - ahead)
                qsend[d - 1, c, :, there] = nn(theirs, a_vm[:, at]).astype(BF)
                put(
                    qsend.at[d - 1, c, :, there], qrecv.at[d - 1, c, :, there], q_left, q_sem.at[d - 1, i],
                    row_from(d), col,
                )

    for h in range(chains):
        left_later(foth.at[:, 0, h], foth_core_left.at[h])
        left_later(fin.at[0, h], fin_core_left.at[h])

    @pl.when(core == 1)
    def _():
        relay_foth()

    @pl.when(core == 0)
    def _():
        wait_foth()

    send_sums(1)

    @pl.when(core == 1)
    def _():
        relay_fin()
        wait_foth()

    @pl.when(core == 0)
    def _():
        relay_foth()
        relay_fin()

    send_sums(0)
    left_later(qsend, q_left)

    for h in range(chains):
        took(fin.at[0, h], fin_core.at[h])
    took(cur_recv.at[0], cur_sem)

    own = joined(fin, x, blocks)
    last_hi, last_lo = split(jnp.concatenate([cur_recv[0], cur_recv[1]], axis=0))

    def finish(at, extra):
        marked = onehot[iters - 2, :, at]
        stepped = nn(last_hi, marked) + nn(last_lo, marked)
        stepped = stepped + STEP_SIZE * (nn(own, a_vm[:, at]) + extra)
        out_ref[:, at] = stepped * keep[:, at]
        squares = jnp.sum(stepped * stepped, axis=0, keepdims=True)
        for j in range(at.start // 128, at.stop // 128):
            nrm_send[j] = squares[:, j * 128 - at.start:(j + 1) * 128 - at.start]

    if ahead:
        took(a_peer, ap_sem)
        peers = [joined(fin, row_from(d), blocks) for d in range(1, n_row)]
        for at in cut(0, ahead):
            finish(at, sum(nn(peers[d - 1], a_peer[d - 1, :, at]) for d in range(1, n_row)))
        for d in range(1, n_row):
            piece = pl.ds(0, near)
            put(nrm_send.at[piece], nrm_recv.at[d - 1, piece], nrm_left.at[0], nrm_sem.at[0], row_at(d), col)
        left_later(nrm_recv.at[:, pl.ds(0, near)], nrm_left.at[0])
        left_later(a_peer, ap_left)

    took(e_recv, e_sem.at[0])
    total = e_send[...] + sum(e_recv[k] for k in range(n_row * chips - 1))
    e_both[0] = total
    put(e_both.at[0], e_both.at[1], e_left.at[1], e_sem.at[1], x, partner)
    left_later(e_both.at[0], e_left.at[1])

    for i, at in enumerate(spans):
        there = slice(at.start - ahead, at.stop - ahead)
        for d in range(1, n_row):
            took(qrecv.at[d - 1, :, :, there], q_sem.at[d - 1, i])
        finish(at, sum(
            jnp.concatenate([qrecv[d - 1, c, :, there] for c in range(2)], axis=0).astype(F32)
            for d in range(1, n_row)
        ))
    for d in range(1, n_row):
        piece = pl.ds(near, lines - near)
        put(nrm_send.at[piece], nrm_recv.at[d - 1, piece], nrm_left.at[1], nrm_sem.at[1], row_at(d), col)
    left_later(nrm_recv.at[:, pl.ds(near, lines - near)], nrm_left.at[1])

    took(e_both.at[1], e_sem.at[1])
    for t in range(iters):
        sums_ref[columns // 128 + t:columns // 128 + t + 1] = e_both[0, t] + e_both[1, t]
    if ahead:
        took(nrm_recv.at[:, pl.ds(0, near)], nrm_sem.at[0])
    took(nrm_recv.at[:, pl.ds(near, lines - near)], nrm_sem.at[1])
    for i in range(lines):
        squares = nrm_send[i] + sum(nrm_recv[d - 1, i] for d in range(1, n_row))
        sums_ref[i:i + 1] = jnp.sqrt(squares)

    for ref, sem in sent:
        took(ref, sem)

    @pl.when(owner_row == x)
    def _():
        for h in range(chains):
            for d in range(1, n_row):
                mp_copy(d, h).wait_send()

    @pl.when(to_row != x)
    def _():
        for h in range(chains):
            first_copy(h).wait_send()

    @pl.when(away > 0)
    def _():
        for h in range(chains):
            took(fin.at[0, h], foth_left.at[h])


def deliver(entries, est_ref, sums_ref, est_out, norm_out, energy_out, sem):
    parts = 8
    rows = est_ref.shape[0] // parts
    lines = norm_out.shape[0]
    copies = [pltpu.make_async_copy(sums_ref.at[pl.ds(0, lines)], norm_out, sem.at[parts])] + [
        pltpu.make_async_copy(
            est_ref.at[pl.ds(i * rows, rows)], est_out.at[pl.ds(i * rows, rows)], sem.at[i]
        )
        for i in range(parts)
    ]
    for copy in copies:
        copy.start()
    for t in range(energy_out.shape[0]):
        energy_out[t] = jnp.sum(sums_ref[lines + t:lines + t + 1]) / entries
    for copy in copies:
        copy.wait()


def local(matrix, measured, support):
    signals, mb = measured.shape
    columns = matrix.shape[1]
    iters = support.shape[0]
    n_row = lax.axis_size("row")
    n_col = lax.axis_size("col")
    s = sizes(n_row, n_col, signals, mb, columns, iters)
    chips, mine, ps, pm, gs, gr, half = (s[k] for k in ("chips", "mine", "ps", "pm", "gs", "gr", "half"))
    chains = s["chains"]
    late = len(cut(s["ahead"], columns))
    rest = columns - s["ahead"]
    lines = columns // 128
    peers = n_row - 1
    dma = pltpu.SemaphoreType.DMA
    vm = pltpu.VMEM
    outs = pl.pallas_call(
        functools.partial(kernel, s),
        out_shape=(
            pltpu.VMEM((half, columns), F32),
            pltpu.VMEM((columns // 128 + (iters + 7) // 8 * 8, 128), F32),
        ),
        in_specs=[
            pl.BlockSpec(memory_space=pltpu.HBM),
            pl.BlockSpec(memory_space=pltpu.HBM),
            pl.BlockSpec(memory_space=pltpu.HBM),
        ],
        out_specs=(pl.BlockSpec(memory_space=vm), pl.BlockSpec(memory_space=vm)),
        scratch_shapes=[
            vm((mb, columns), BF),
            vm(support.shape, support.dtype),
            vm(measured.shape, F32),
            vm((chains, ps, pm), F32),
            vm((iters - 1, KMAX, columns), BF),
            vm((iters - 1, 2 * KMAX, 2 * KMAX), BF),
            vm((iters - 1, n_row, 2 * KMAX, mb), BF),
            vm((2, n_row, mine, KMAX), BF),
            vm((2 * n_row, n_row, mine, KMAX), BF),
            vm((iters - 1, chains, chips, ps, pm), BF),
            vm((iters - 1, chains, chips - 1, ps, pm), BF),
            vm((chains, ps, pm), BF),
            vm((iters - 1, chains, chips, ps, pm), BF),
            vm((2, chains, chips, ps, pm), BF),
            vm((peers, 2, chains, gs * gr, ps, pm), BF),
            vm((2, mine, KMAX), F32),
            vm((2, mine, KMAX), F32),
            vm((peers, 2, mine, rest), BF),
            vm((peers, 2, mine, rest), BF),
            vm((peers, mb, max(s["ahead"], 128)), BF),
            vm((lines, 1, 128), F32),
            vm((peers, lines, 1, 128), F32),
            vm((iters, 1, 128), F32),
            vm((n_row * chips - 1, iters, 1, 128), F32),
            vm((2, iters, 1, 128), F32),
            dma((2,)),
            dma((4,)),
            dma((chains,)),
            dma((peers, chains)),
            dma((iters - 1, 3)),
            dma,
            dma((iters - 1, chains)),
            dma((iters - 1, chains)),
            dma((chains,)),
            dma((chains,)),
            dma((chains,)),
            dma((chains,)),
            dma((chains,)),
            dma,
            dma,
            dma,
            dma((2,)),
            dma((2,)),
            dma((iters - 1, peers)),
            dma((iters - 1, n_row)),
            dma,
            dma((iters - 1, chains)),
            dma((iters - 1, chains)),
            dma((chains,)),
            dma((chains,)),
            dma((chains,)),
            dma((chains, peers)),
            dma,
            dma((peers, late)),
            dma,
            dma((2,)),
            dma((2,)),
        ],
        compiler_params=pltpu.CompilerParams(
            collective_id=0, has_side_effects=True, vmem_limit_bytes=60 * 1024 * 1024
        ),
    )(support, measured, matrix)
    estimate, norms, energy = pl.pallas_call(
        functools.partial(deliver, signals * mb * n_row),
        out_shape=(
            jax.ShapeDtypeStruct((half, columns), F32),
            jax.ShapeDtypeStruct((columns // 128, 128), F32),
            jax.ShapeDtypeStruct((iters,), F32),
        ),
        in_specs=[pl.BlockSpec(memory_space=vm), pl.BlockSpec(memory_space=vm)],
        out_specs=(
            pl.BlockSpec(memory_space=pltpu.HBM), pl.BlockSpec(memory_space=pltpu.HBM),
            pl.BlockSpec(memory_space=pltpu.SMEM),
        ),
        scratch_shapes=[dma((9,))],
        compiler_params=pltpu.CompilerParams(vmem_limit_bytes=8 * 1024 * 1024),
    )(*outs)
    return estimate, norms.reshape(columns), energy


def solution(mesh):
    placed = (P("row", "col"), P(None, "row"), P())
    return jax.shard_map(
        local,
        mesh=mesh,
        in_specs=placed,
        out_specs=(P("row", "col"), P("col"), P()),
        check_vma=False,
    )
```
